32 devices in a mesh: lon: 8 (over z, x), lat: 4 (over y, core).
Axes of the slice: x: 2, y: 2, z: 4, core: 2. Of those that a mesh axis runs over, the one named last changes fastest.
Arguments:
- thermal_anomaly: float32 [32, 64, 512], P(None, 'lon', 'lat'), may hold values from -5 to 5
- saltiness_anomaly: float32 [32, 64, 512], P(None, 'lon', 'lat'), may hold values from -5 to 5
- zonal_flow: float32 [32, 64, 512], P(None, 'lon', 'lat'), may hold values from -1.2 to 1.2
- meridional_flow: float32 [32, 64, 512], P(None, 'lon', 'lat'), may hold values from -1.2 to 1.2
- submerged_strata_number: int32 [64, 512], P('lon', 'lat'), may hold values from 1 to 32
- sea_indicator: int32 [64, 512], P('lon', 'lat'), may hold values 0 or 1
- strata_thickness: float32 [32], replicated, may hold values from 0.5 to 2
- earlier_sea_elevation: float32 [64, 512], P('lon', 'lat'), may hold values from -3 to 3
- sea_drive_term: float32 [64, 512], P('lon', 'lat'), may hold values from -10 to 10
Outputs:
- new_temperature: float32 [32, 64, 512], P(None, 'lon', 'lat')
- new_salinity: float32 [32, 64, 512], P(None, 'lon', 'lat')
- new_u_velocity: float32 [32, 64, 512], P(None, 'lon', 'lat')
- new_v_velocity: float32 [32, 64, 512], P(None, 'lon', 'lat')
- new_surface: float32 [64, 512], P('lon', 'lat')
- residual_rms: float32 [], replicated
The draws below stay inside these ranges and needn't reach their ends.
All inputs are finite; a program needn't handle non-finite values. No bound on the sum of `sea_indicator` on one device may be relied on, other than what follows from the above.
Results may differ from the reference program's by a relative error of at most 0.0003.
Values sent between devices are 32-bit elements; how exact they have to be, the bound alone decides.
A program may use at most 128 MiB of HBM per device.

```python
import math
import jax
import jax.numpy as jnp
from jax import lax

STRATA_TOTAL = 32
CLON = 8
ITERS = 4
ZONAL_POINTS = 64
MERIDIAN_ROWS = 512
N_LON = 8


def draw_sea_drive_term(key, part):
    key_rough = jax.random.fold_in(jax.random.fold_in(key, 11), 0)
    growth = 1.0 + 2.0 * jnp.arange(ZONAL_POINTS, dtype=jnp.float32)[:, None] / (ZONAL_POINTS - 1)
    random_part = jnp.clip(jax.random.normal(key_rough, (ZONAL_POINTS, MERIDIAN_ROWS), jnp.float32), -4.0, 4.0)
    return 0.5 * growth * random_part


def touch_ends(result, key, smallest, top_value):
    shape = result.shape
    spot = [jax.random.randint(jax.random.fold_in(key, axis), (), 0, shape[axis]) for axis in range(len(shape))]
    result = result.at[tuple(spot)].set(smallest)
    longest = shape.index(max(shape))
    spot[longest] = (spot[longest] + 1) % shape[longest]
    return result.at[tuple(spot)].set(top_value)


def block_scale(key, shape, pieces, low, high):
    gain, own = 1.0, jax.random.fold_in(key, 6)
    for axis_at, shards_of in pieces:
        steps = jnp.exp(jax.random.uniform(jax.random.fold_in(own, axis_at), (shards_of,), jnp.float32, low / len(pieces), high / len(pieces)))
        gain = gain * jnp.repeat(steps, shape[axis_at] // shards_of).reshape([-1 if axis == axis_at else 1 for axis in range(len(shape))])
    return gain


def normal_values(rng, dims, scale, limit, shards=(), kind=jnp.bfloat16):
    entries = scale * jax.random.normal(rng, dims, jnp.float32)
    if shards:
        entries = entries * block_scale(rng, dims, shards, -0.22, 0.18)
    return jnp.clip(entries, -limit, limit).astype(kind)


def setup_inputs(seed: int = 0) -> dict:
    streams_of = jax.random.split(jax.random.key(seed), 10)
    return {
        "thermal_anomaly": normal_values(streams_of[0], (STRATA_TOTAL, ZONAL_POINTS, MERIDIAN_ROWS), 1.0, 5.0, ((1, 8), (2, 4)), jnp.float32),
        "saltiness_anomaly": normal_values(streams_of[1], (STRATA_TOTAL, ZONAL_POINTS, MERIDIAN_ROWS), 1.0, 5.0, ((1, 8), (2, 4)), jnp.float32),
        "zonal_flow": normal_values(streams_of[2], (STRATA_TOTAL, ZONAL_POINTS, MERIDIAN_ROWS), 0.3, 1.2, ((1, 8), (2, 4)), jnp.float32),
        "meridional_flow": normal_values(streams_of[3], (STRATA_TOTAL, ZONAL_POINTS, MERIDIAN_ROWS), 0.3, 1.2, ((1, 8), (2, 4)), jnp.float32),
        "submerged_strata_number": touch_ends(jax.random.randint(streams_of[4], (ZONAL_POINTS, MERIDIAN_ROWS), 1, STRATA_TOTAL + 1), jax.random.fold_in(streams_of[4], 1), 1, STRATA_TOTAL).astype(jnp.int32),
        "sea_indicator": touch_ends((jax.random.randint(streams_of[5], (ZONAL_POINTS, MERIDIAN_ROWS), 0, 5) < 4).astype(jnp.int32), jax.random.fold_in(streams_of[5], 1), 0, 1),
        "strata_thickness": jnp.clip(jnp.exp(jax.random.uniform(streams_of[6], (STRATA_TOTAL,), jnp.float32, math.log(0.5), math.log(2.0))), 0.5, 2.0),
        "earlier_sea_elevation": normal_values(streams_of[7], (ZONAL_POINTS, MERIDIAN_ROWS), 0.5, 3.0, ((0, 8), (1, 4)), jnp.float32),
        "sea_drive_term": draw_sea_drive_term(jax.random.fold_in(streams_of[9], 71), 0),
    }


DIFFUSION = 0.15
MIXING = 0.1
EXPANSION = 0.2
CONTRACTION = 0.15
PRESSURE_SCALE = 0.02
CORIOLIS = 0.5
FRICTION = 0.01
DIVERGENCE = 0.3
STORAGE = 0.1
SPECTRUM_LOW = 0.1
SPECTRUM_HIGH = 1.9
GRAVITY = 0.3
EPSILON = 1e-06

def extend(field, sign_rows, width):
    folded = jnp.flip(field[:, :, MERIDIAN_ROWS - width:], (1, 2)) * sign_rows[:, None, None]
    southern = jnp.zeros((field.shape[0], ZONAL_POINTS, width), field.dtype)
    padded = jnp.concatenate([southern, field, folded], axis=2)
    return jnp.concatenate([padded[:, ZONAL_POINTS - width:], padded, padded[:, :width]], axis=1)

def center(field):
    return field[:, 1:-1, 1:-1]

def to_east(field):
    return field[:, 2:, 1:-1]

def to_west(field):
    return field[:, :-2, 1:-1]

def to_north(field):
    return field[:, 1:-1, 2:]

def to_south(field):
    return field[:, 1:-1, :-2]

def shrink(field):
    return field[:, 1:-1, 1:-1]

def level_mask(strata_bottoms, strata_indices):
    level_index = jnp.arange(strata_indices).astype(strata_bottoms.dtype)[:, None, None]
    return jnp.where(level_index + 0.5 < strata_bottoms, 1.0, 0.0).astype(strata_bottoms.dtype)

def laplace(field, mask):
    middle = center(field)
    total = to_east(mask) * (to_east(field) - middle) + to_west(mask) * (to_west(field) - middle)
    total = total + to_north(mask) * (to_north(field) - middle) + to_south(mask) * (to_south(field) - middle)
    return center(mask) * total

def tracer_step(tracer, u_field, v_field, mask, thickness):
    middle = center(tracer)
    wet_mid = center(mask)
    u_mid = center(u_field)
    v_mid = center(v_field)
    flux_east = wet_mid * to_east(mask) * (0.5 * (u_mid + to_east(u_field)) * 0.5 * (middle + to_east(tracer)) - DIFFUSION * (to_east(tracer) - middle))
    flux_west = wet_mid * to_west(mask) * (0.5 * (to_west(u_field) + u_mid) * 0.5 * (to_west(tracer) + middle) - DIFFUSION * (middle - to_west(tracer)))
    flux_north = wet_mid * to_north(mask) * (0.5 * (v_mid + to_north(v_field)) * 0.5 * (middle + to_north(tracer)) - DIFFUSION * (to_north(tracer) - middle))
    flux_south = wet_mid * to_south(mask) * (0.5 * (to_south(v_field) + v_mid) * 0.5 * (to_south(tracer) + middle) - DIFFUSION * (middle - to_south(tracer)))
    horizontal = flux_west - flux_east + flux_south - flux_north
    spacing = 0.5 * (thickness[1:] + thickness[:-1])
    vflux = wet_mid[1:] * wet_mid[:-1] * (middle[1:] - middle[:-1]) / spacing[:, None, None]
    zero_plane = jnp.zeros_like(middle[:1])
    upper_flux = jnp.concatenate([vflux, zero_plane], axis=0)
    lower_flux = jnp.concatenate([zero_plane, vflux], axis=0)
    vertical = MIXING * (upper_flux - lower_flux) / thickness[:, None, None]
    return wet_mid * (middle + horizontal + vertical)

def pressure_gradients(temp_rim, salt_rim, mask, thickness):
    density = (CONTRACTION * salt_rim - EXPANSION * temp_rim) * thickness[:, None, None] * mask
    pressure = jnp.cumsum(density, axis=0)
    middle = center(pressure)
    wet_mid = center(mask)
    grad_x = 0.5 * wet_mid * (to_east(mask) * (to_east(pressure) - middle) + to_west(mask) * (middle - to_west(pressure)))
    grad_y = 0.5 * wet_mid * (to_north(mask) * (to_north(pressure) - middle) + to_south(mask) * (middle - to_south(pressure)))
    return (grad_x, grad_y)

def baroclinic(narrow, mask_narrow, lap_u, lap_v, thickness, coriolis, strata_indices):
    temp_rim = narrow[:strata_indices]
    salt_rim = narrow[strata_indices:2 * strata_indices]
    u_rim = narrow[2 * strata_indices:3 * strata_indices]
    v_rim = narrow[3 * strata_indices:4 * strata_indices]
    new_temp = tracer_step(temp_rim, u_rim, v_rim, mask_narrow, thickness)
    new_salt = tracer_step(salt_rim, u_rim, v_rim, mask_narrow, thickness)
    grad_x, grad_y = pressure_gradients(temp_rim, salt_rim, mask_narrow, thickness)
    friction_u = laplace(lap_u, mask_narrow)
    friction_v = laplace(lap_v, mask_narrow)
    wet_mid = center(mask_narrow)
    u_mid = center(u_rim)
    v_mid = center(v_rim)
    u_star = wet_mid * (u_mid + coriolis * v_mid - PRESSURE_SCALE * grad_x - FRICTION * friction_u)
    v_star = wet_mid * (v_mid - coriolis * u_mid - PRESSURE_SCALE * grad_y - FRICTION * friction_v)
    height = lax.optimization_barrier(jnp.sum(thickness[:, None, None] * mask_narrow, axis=0, keepdims=True))
    return (new_temp, new_salt, u_star, v_star, height, wet_mid)

def solver_weights(height, strata_indices):
    middle = center(height)
    w_east = jnp.minimum(middle, to_east(height)) / strata_indices
    w_west = jnp.minimum(middle, to_west(height)) / strata_indices
    w_north = jnp.minimum(middle, to_north(height)) / strata_indices
    w_south = jnp.minimum(middle, to_south(height)) / strata_indices
    diagonal = STORAGE + w_east + w_west + w_north + w_south
    return (w_east, w_west, w_north, w_south, diagonal)

def apply_operator(weights, field_rim):
    w_east, w_west, w_north, w_south, diagonal = weights
    coupled = w_east * to_east(field_rim) + w_west * to_west(field_rim) + w_north * to_north(field_rim) + w_south * to_south(field_rim)
    return diagonal * center(field_rim) - coupled

def line_factor(w_west, w_east, diagonal):
    count = diagonal.shape[0]
    position = jnp.arange(count).reshape((count,) + (1,) * (diagonal.ndim - 1))
    lower_band = jnp.where(position > 0, -w_west, 0.0)
    upper_band = jnp.where(position < count - 1, -w_east, 0.0)

    def forward(previous, inputs):
        lower_row, diag_row, upper_row = inputs
        inverse = 1.0 / (diag_row - lower_row * previous)
        factor = upper_row * inverse
        return (factor, (factor, inverse))
    _, (factors, pivots) = lax.scan(forward, jnp.zeros_like(diagonal[0]), (lower_band, diagonal, upper_band))
    return (lower_band, factors, pivots)

def line_solve(lower_band, factors, pivots, values):

    def forward(previous, inputs):
        lower_row, inverse, value_row = inputs
        current = (value_row - lower_row * previous) * inverse
        return (current, current)
    _, partial_rows = lax.scan(forward, jnp.zeros_like(values[0]), (lower_band, pivots, values))

    def backward(following, inputs):
        factor, partial_row = inputs
        current = partial_row - factor * following
        return (current, current)
    _, solved = lax.scan(backward, jnp.zeros_like(values[0]), (factors, partial_rows), reverse=True)
    return solved

def to_lines(field):
    return jnp.transpose(field.reshape(N_LON, CLON, MERIDIAN_ROWS), (1, 0, 2))

def from_lines(field):
    return jnp.transpose(field, (1, 0, 2)).reshape(ZONAL_POINTS, MERIDIAN_ROWS)

def reference(thermal_anomaly, saltiness_anomaly, zonal_flow, meridional_flow, submerged_strata_number, sea_indicator, strata_thickness, earlier_sea_elevation, sea_drive_term):
    strata_indices = thermal_anomaly.shape[0]
    real_number_kind = thermal_anomaly.dtype
    wet_surface = sea_indicator.astype(real_number_kind)
    strata_bottoms = (submerged_strata_number * sea_indicator).astype(real_number_kind)[None]
    joined_tracers = jnp.concatenate([thermal_anomaly, saltiness_anomaly, zonal_flow, meridional_flow, strata_bottoms], axis=0)
    sign_rows = jnp.concatenate([jnp.ones(2 * strata_indices, real_number_kind), -jnp.ones(2 * strata_indices, real_number_kind), jnp.ones(1, real_number_kind)])
    wide_rim = extend(joined_tracers, sign_rows, 2)
    mask_wide = level_mask(wide_rim[4 * strata_indices:], strata_indices)
    narrow = shrink(wide_rim)
    mask_narrow = shrink(mask_wide)
    lap_u = laplace(wide_rim[2 * strata_indices:3 * strata_indices], mask_wide)
    lap_v = laplace(wide_rim[3 * strata_indices:4 * strata_indices], mask_wide)
    lat_index = jnp.arange(MERIDIAN_ROWS).astype(real_number_kind)
    coriolis = CORIOLIS * (2.0 * (lat_index + 0.5) / MERIDIAN_ROWS - 1.0)
    new_temp, new_salt, u_star, v_star, height, wet_mid = baroclinic(narrow, mask_narrow, lap_u, lap_v, strata_thickness, coriolis, strata_indices)
    weights = solver_weights(height, strata_indices)
    lower_band, factors, pivots = line_factor(to_lines(weights[1][0]), to_lines(weights[0][0]), to_lines(weights[4][0]))

    def precondition(values):
        return from_lines(line_solve(lower_band, factors, pivots, to_lines(values[0])))[None]
    transport_u = lax.optimization_barrier(jnp.sum(strata_thickness[:, None, None] * u_star, axis=0, keepdims=True))
    transport_v = lax.optimization_barrier(jnp.sum(strata_thickness[:, None, None] * v_star, axis=0, keepdims=True))
    start_field = (wet_surface * earlier_sea_elevation)[None]
    surface_signs = jnp.array([-1.0, -1.0, 1.0], real_number_kind)
    plus_one = jnp.ones(1, real_number_kind)
    moved = extend(jnp.concatenate([transport_u, transport_v, start_field], axis=0), surface_signs, 1)
    divergence = 0.5 * (to_east(moved[0:1]) - to_west(moved[0:1])) + 0.5 * (to_north(moved[1:2]) - to_south(moved[1:2]))
    right_side = wet_surface[None] * (sea_drive_term[None] - DIVERGENCE * divergence)
    solution = center(moved[2:3])
    residual = right_side - apply_operator(weights, moved[2:3])
    spectrum_mid = 0.5 * (SPECTRUM_HIGH + SPECTRUM_LOW)
    spectrum_half = 0.5 * (SPECTRUM_HIGH - SPECTRUM_LOW)
    spectrum_ratio = spectrum_mid / spectrum_half
    direction = precondition(residual) / spectrum_mid
    cheby_rho = 1.0 / spectrum_ratio
    for step_index in range(ITERS):
        solution = solution + direction
        if step_index + 1 < ITERS:
            residual = residual - apply_operator(weights, extend(direction, plus_one, 1))
            rho_next = 1.0 / (2.0 * spectrum_ratio - cheby_rho)
            direction = rho_next * cheby_rho * direction + 2.0 * rho_next / spectrum_half * precondition(residual)
            cheby_rho = rho_next
    final_rim = extend(solution, plus_one, 1)
    final_residual = right_side - apply_operator(weights, final_rim)
    residual_rms = jnp.sqrt(jnp.sum(final_residual * final_residual) / (ZONAL_POINTS * MERIDIAN_ROWS) + EPSILON)
    slope_x = 0.5 * (to_east(final_rim) - to_west(final_rim))
    slope_y = 0.5 * (to_north(final_rim) - to_south(final_rim))
    new_u = wet_mid * (u_star - GRAVITY * slope_x)
    new_v = wet_mid * (v_star - GRAVITY * slope_y)
    return (new_temp, new_salt, new_u, new_v, solution[0], residual_rms)
```

```python
import functools

import jax
import jax.numpy as jnp
from jax import lax
from jax.experimental import pallas as pl
from jax.experimental.pallas import tpu as pltpu
from jax.sharding import PartitionSpec as P

ITERS = 4
DIFFUSION = 0.15
MIXING = 0.1
EXPANSION = 0.2
CONTRACTION = 0.15
PRESSURE_SCALE = 0.02
CORIOLIS = 0.5
FRICTION = 0.01
DIVERGENCE = 0.3
STORAGE = 0.1
SPECTRUM_LOW = 0.1
SPECTRUM_HIGH = 1.9
GRAVITY = 0.3
EPSILON = 1e-06

MESH = pl.DeviceIdType.MESH
F32 = jnp.float32
SLOT_N, SLOT_NE, SLOT_NW, SLOT_S, SLOT_SE, SLOT_SW = range(6)
SEM_E, SEM_W = 6, 7
FIELDS = 5


def iota(shape, axis):
    return lax.broadcasted_iota(jnp.int32, shape, axis)


def flip_rows(x):
    n = x.shape[0]
    row = iota(x.shape, 0)
    bit = n // 2
    while bit:
        up = pltpu.roll(x, bit, 0)
        down = pltpu.roll(x, n - bit, 0)
        x = up if 2 * bit == n else jnp.where((row & bit) != 0, up, down)
        bit //= 2
    return x


def step_kernel(n_lon, n_lat, t_ref, s_ref, u_ref, v_ref, num_ref, sea_ref, thick_ref, eta_ref,
                drive_ref, ot_ref, os_ref, ou_ref, ov_ref, op_ref, epk, wpk, npk, spk, slot_e,
                slot_w, slots, rim, send_sem, recv_sem):
    K, NI, NJ = t_ref.shape
    p = lax.axis_index("lon")
    q = lax.axis_index("lat")
    east_dev = lax.rem(p + 1, n_lon)
    west_dev = lax.rem(p + n_lon - 1, n_lon)
    at_pole = q == n_lat - 1
    not_pole = q < n_lat - 1
    not_south = q > 0
    mirror = n_lon - 1 - p
    mirror_ne = lax.rem(2 * n_lon - 2 - p, n_lon)
    mirror_nw = lax.rem(2 * n_lon - p, n_lon)
    ne_remote = jnp.logical_or(not_pole, mirror_ne != p)
    nw_remote = jnp.logical_or(not_pole, mirror_nw != p)
    ne_self = jnp.logical_and(at_pole, mirror_ne == p)
    nw_self = jnp.logical_and(at_pole, mirror_nw == p)

    barrier = pltpu.get_barrier_semaphore()

    def greet(lon, lat):
        pl.semaphore_signal(barrier, inc=1, device_id={"lon": lon, "lat": lat}, device_id_type=MESH)

    greet(east_dev, q)
    greet(west_dev, q)

    @pl.when(not_south)
    def _():
        for lon in (p, east_dev, west_dev):
            greet(lon, q - 1)

    @pl.when(not_pole)
    def _():
        for lon in (p, east_dev, west_dev):
            greet(lon, q + 1)

    @pl.when(at_pole)
    def _():
        greet(mirror, q)

    @pl.when(jnp.logical_and(at_pole, mirror_ne != p))
    def _():
        greet(mirror_ne, q)

    @pl.when(jnp.logical_and(at_pole, mirror_nw != p))
    def _():
        greet(mirror_nw, q)

    sub = iota((NI, NJ), 0)
    lane = iota((NI, NJ), 1)
    depth = (num_ref[...] * sea_ref[...]).astype(F32)

    fields = (t_ref, s_ref, u_ref, v_ref)
    for pk, d1, d2 in ((epk, NI - 1, NI - 2), (wpk, 0, 1)):
        for f, ref in enumerate(fields):
            pk[f * K:(f + 1) * K, :] = ref[:, d1, :]
        pk[4 * K:5 * K, :] = u_ref[:, d2, :]
        pk[5 * K:6 * K, :] = v_ref[:, d2, :]
        pk[6 * K:6 * K + NI, :] = jnp.zeros((NI, NJ), F32)
        pk[6 * K:6 * K + 1, :] = depth[d1:d1 + 1, :]
        pk[6 * K + 1:6 * K + 2, :] = depth[d2:d2 + 1, :]

    n0 = jnp.zeros((NI, NJ), F32)
    s0 = jnp.zeros((NI, NJ), F32)
    n1 = jnp.zeros((NI, NJ), F32)
    s1 = jnp.zeros((NI, NJ), F32)

    def put(acc, x, source, target):
        moved = pltpu.roll(x, (target - source) % NJ, 1) if source != target else x
        return jnp.where(lane == target, moved, acc)

    for f, ref in enumerate(fields):
        for k in range(K):
            x = ref[k]
            target = f * K + k
            n0 = put(n0, x, NJ - 1, target)
            s0 = put(s0, x, 0, target)
            if f >= 2:
                n1 = put(n1, x, NJ - 2, target)
                s1 = put(s1, x, 1, target)
    n1 = put(put(n1, depth, NJ - 1, 0), depth, NJ - 2, 1)
    s1 = put(put(s1, depth, 0, 0), depth, 1, 1)
    npk[0] = n0
    npk[1] = n1
    spk[0] = s0
    spk[1] = s1

    peers = (3 + 2 * not_pole.astype(jnp.int32) + 3 * not_south.astype(jnp.int32)
             + at_pole.astype(jnp.int32) * ((mirror_ne != p).astype(jnp.int32) + (mirror_nw != p).astype(jnp.int32)))
    pl.semaphore_wait(barrier, peers)

    def copy(src, dst, lon, lat, out, into):
        return pltpu.make_async_remote_copy(
            src_ref=src, dst_ref=dst, send_sem=send_sem.at[out], recv_sem=recv_sem.at[into],
            device_id={"lon": lon, "lat": lat}, device_id_type=MESH)

    def edge(src, slot, lon, lat, out):
        return copy(src, slots.at[slot], lon, lat, out, slot)

    to_east = copy(epk, slot_w, east_dev, q, SEM_E, SEM_W)
    to_west = copy(wpk, slot_e, west_dev, q, SEM_W, SEM_E)
    to_east.start()
    to_west.start()

    @pl.when(not_south)
    def _():
        edge(spk, SLOT_N, p, q - 1, SLOT_S).start()
        edge(spk, SLOT_NW, east_dev, q - 1, SLOT_SE).start()
        edge(spk, SLOT_NE, west_dev, q - 1, SLOT_SW).start()

    @pl.when(not_pole)
    def _():
        edge(npk, SLOT_S, p, q + 1, SLOT_N).start()
        edge(npk, SLOT_SW, east_dev, q + 1, SLOT_NE).start()
        edge(npk, SLOT_SE, west_dev, q + 1, SLOT_NW).start()

    @pl.when(at_pole)
    def _():
        edge(npk, SLOT_N, mirror, q, SLOT_N).start()

    @pl.when(jnp.logical_and(at_pole, mirror_ne != p))
    def _():
        edge(npk, SLOT_NE, mirror_ne, q, SLOT_NE).start()

    @pl.when(jnp.logical_and(at_pole, mirror_nw != p))
    def _():
        edge(npk, SLOT_NW, mirror_nw, q, SLOT_NW).start()

    edge(npk, SLOT_N, p, q, SLOT_N).wait_recv()

    @pl.when(ne_remote)
    def _():
        edge(npk, SLOT_NE, p, q, SLOT_NE).wait_recv()

    @pl.when(nw_remote)
    def _():
        edge(npk, SLOT_NW, p, q, SLOT_NW).wait_recv()

    @pl.when(not_south)
    def _():
        for slot in (SLOT_S, SLOT_SE, SLOT_SW):
            edge(spk, slot, p, q, slot).wait_recv()

    sign = jnp.where(lane >= 2 * K, -1.0, 1.0).astype(F32)

    def northern(slot, own):
        out = []
        for i in range(2):
            x = slots[slot, i]
            if own is not None:
                x = jnp.where(own, npk[i], x)
            out.append(jnp.where(at_pole, flip_rows(x) * sign, x))
        return out

    def southern(slot):
        return [jnp.where(not_south, slots[slot, i], 0.0) for i in range(2)]

    pn0, pn1 = northern(SLOT_N, None)
    pne0, pne1 = northern(SLOT_NE, ne_self)
    pnw0, pnw1 = northern(SLOT_NW, nw_self)
    ps0, ps1 = southern(SLOT_S)
    pse0, pse1 = southern(SLOT_SE)
    psw0, psw1 = southern(SLOT_SW)

    def shift_e(x, row):
        return jnp.where(sub == NI - 1, row, pltpu.roll(x, NI - 1, 0))

    def shift_w(x, row):
        return jnp.where(sub == 0, row, pltpu.roll(x, 1, 0))

    level_l = (lane - K * (lane // K)).astype(F32) + 0.5

    def wet_l(d):
        return jnp.where(level_l < d, 1.0, 0.0)

    def spread(x, i):
        return jnp.broadcast_to(x[:, i:i + 1], (NI, NJ))

    def packed_lap(c0, c1, e0, e1, w0, w1, own, own_depth):
        d = spread(c1, 0)
        de = shift_e(d, jnp.broadcast_to(e1[0:1, 0:1], (NI, NJ)))
        dw = shift_w(d, jnp.broadcast_to(w1[NI - 1:NI, 0:1], (NI, NJ)))
        xe = shift_e(c0, jnp.broadcast_to(e0[0:1, :], (NI, NJ)))
        xw = shift_w(c0, jnp.broadcast_to(w0[NI - 1:NI, :], (NI, NJ)))
        total = wet_l(de) * (xe - c0) + wet_l(dw) * (xw - c0)
        total = total + wet_l(spread(c1, 1)) * (c1 - c0) + wet_l(own_depth) * (own - c0)
        return wet_l(d) * total

    lap_n = packed_lap(pn0, pn1, pne0, pne1, pnw0, pnw1, n0, spread(depth, NJ - 1))
    lap_s = packed_lap(ps0, ps1, pse0, pse1, psw0, psw1, s0, spread(depth, 0))
    rim[4, 0:NI, :] = lap_n
    rim[5, 0:NI, :] = lap_s
    rim[4, NI:2 * NI, :] = pn0
    rim[5, NI:2 * NI, :] = ps0

    to_east.wait_recv()
    to_west.wait_recv()

    level_r = iota((K, NJ), 0)
    lane_r = iota((K, NJ), 1)
    level_rf = level_r.astype(F32) + 0.5

    def wet_r(d):
        return jnp.where(level_rf < d, 1.0, 0.0)

    def wide(row):
        return jnp.broadcast_to(row, (K, NJ))

    for side, (slot, pk, d1, cn0, cn1, cs0, cs1) in enumerate((
            (slot_e, epk, NI - 1, pne0[0:1], pne1[0:1], pse0[0:1], pse1[0:1]),
            (slot_w, wpk, 0, pnw0[NI - 1:], pnw1[NI - 1:], psw0[NI - 1:], psw1[NI - 1:]))):
        d = wide(slot[6 * K:6 * K + 1, :])
        far = wet_r(wide(slot[6 * K + 1:6 * K + 2, :]))
        own = wet_r(wide(depth[d1:d1 + 1, :]))
        dn = jnp.where(lane_r == NJ - 1, jnp.broadcast_to(cn1[:, 0:1], (K, NJ)), pltpu.roll(d, NJ - 1, 1))
        ds = jnp.where(lane_r == 0, jnp.broadcast_to(cs1[:, 0:1], (K, NJ)), pltpu.roll(d, 1, 1))
        mid, mn, ms = wet_r(d), wet_r(dn), wet_r(ds)
        for i in range(2):
            f = 2 + i
            x = slot[f * K:(f + 1) * K, :]
            pick = lane_r == level_r + f * K
            cn = jnp.sum(jnp.where(pick, wide(cn0), 0.0), axis=1, keepdims=True)
            cs = jnp.sum(jnp.where(pick, wide(cs0), 0.0), axis=1, keepdims=True)
            xn = jnp.where(lane_r == NJ - 1, jnp.broadcast_to(cn, (K, NJ)), pltpu.roll(x, NJ - 1, 1))
            xs = jnp.where(lane_r == 0, jnp.broadcast_to(cs, (K, NJ)), pltpu.roll(x, 1, 1))
            total = far * (slot[(4 + i) * K:(5 + i) * K, :] - x) + own * (pk[f * K:(f + 1) * K, :] - x)
            total = total + mn * (xn - x) + ms * (xs - x)
            rim[2 * side + i] = mid * total

    def shift_n(x, packed, source):
        return jnp.where(lane == NJ - 1, pltpu.roll(packed, NJ - 1 - source, 1), pltpu.roll(x, NJ - 1, 1))

    def shift_s(x, packed, source):
        return jnp.where(lane == 0, pltpu.roll(packed, lax.rem(NJ - source, NJ), 1), pltpu.roll(x, 1, 1))

    depth_e = shift_e(depth, slot_e[6 * K:6 * K + 1, :])
    depth_w = shift_w(depth, slot_w[6 * K:6 * K + 1, :])
    depth_n = shift_n(depth, pn1, 0)
    depth_s = jnp.where(lane == 0, ps1, pltpu.roll(depth, 1, 1))
    both_e = jnp.minimum(depth, depth_e)
    both_w = jnp.minimum(depth, depth_w)
    both_n = jnp.minimum(depth, depth_n)
    both_s = jnp.minimum(depth, depth_s)
    lat_index = (q * NJ + lane).astype(F32)
    coriolis = CORIOLIS * (2.0 * (lat_index + 0.5) / (n_lat * NJ) - 1.0)

    zero = jnp.zeros((NI, NJ), F32)

    def level(k, carry):
        pc, pe, pw, pn_, ps_, flux_t, flux_s, tu, tv, height = carry
        kf = lax.convert_element_type(k, F32) + 0.5
        h = thick_ref[k]
        nxt = jnp.minimum(k + 1, K - 1)
        h_next = thick_ref[nxt]
        hv = jnp.full((NI, NJ), h, F32)
        inv_space = 1.0 / (0.5 * (hv + h_next))
        inv_h = MIXING / hv

        def wet(d):
            return jnp.where(d > kf, 1.0, 0.0)

        mc = wet(depth)
        me, mw, mn, ms = wet(both_e), wet(both_w), wet(both_n), wet(both_s)
        below = jnp.where(jnp.logical_and(depth > kf + 1.0, k < K - 1), inv_space, 0.0)
        pn0v = rim[4, NI:2 * NI, :]
        ps0v = rim[5, NI:2 * NI, :]
        lapn = rim[4, 0:NI, :]
        laps = rim[5, 0:NI, :]

        def around(ref, f):
            x = ref[k]
            row = pl.ds(f * K + k, 1)
            return (x, shift_e(x, slot_e[row, :]), shift_w(x, slot_w[row, :]),
                    shift_n(x, pn0v, f * K + k), shift_s(x, ps0v, f * K + k))

        t = around(t_ref, 0)
        s = around(s_ref, 1)
        u = around(u_ref, 2)
        v = around(v_ref, 3)
        ae = 0.25 * me * (u[0] + u[1])
        aw = 0.25 * mw * (u[0] + u[2])
        an = 0.25 * mn * (v[0] + v[3])
        as_ = 0.25 * ms * (v[0] + v[4])
        ge, gw, gn, gs = DIFFUSION * me, DIFFUSION * mw, DIFFUSION * mn, DIFFUSION * ms

        def tracer(x, ref, flux_above):
            c, e, w, n, so = x
            total = aw * (w + c) - gw * (c - w) - ae * (c + e) + ge * (e - c)
            total = total + as_ * (so + c) - gs * (c - so) - an * (c + n) + gn * (n - c)
            flux = below * (ref[nxt] - c)
            return mc * (c + total + inv_h * (flux - flux_above)), flux

        new_t, flux_t = tracer(t, t_ref, flux_t)
        new_s, flux_s = tracer(s, s_ref, flux_s)
        ot_ref[k] = new_t
        os_ref[k] = new_s
        pressures = []
        for i, (acc, d) in enumerate(((pc, depth), (pe, depth_e), (pw, depth_w), (pn_, depth_n), (ps_, depth_s))):
            density = CONTRACTION * s[i] - EXPANSION * t[i]
            pressures.append(acc + jnp.where(d > kf, density * h, 0.0))
        pc, pe, pw, pn_, ps_ = pressures
        grad_x = 0.5 * (me * (pe - pc) + mw * (pc - pw))
        grad_y = 0.5 * (mn * (pn_ - pc) + ms * (pc - ps_))

        def biharmonic(x, i):
            c, e, w, n, so = x
            lap = me * (e - c) + mw * (w - c) + mn * (n - c) + ms * (so - c)
            row = pl.ds(k, 1)
            le = shift_e(lap, rim[i, row, :])
            lw = shift_w(lap, rim[2 + i, row, :])
            source = (2 + i) * K + k
            ln = shift_n(lap, lapn, source)
            ls = shift_s(lap, laps, source)
            return me * (le - lap) + mw * (lw - lap) + mn * (ln - lap) + ms * (ls - lap)

        u_star = mc * (u[0] + coriolis * v[0] - PRESSURE_SCALE * grad_x - FRICTION * biharmonic(u, 0))
        v_star = mc * (v[0] - coriolis * u[0] - PRESSURE_SCALE * grad_y - FRICTION * biharmonic(v, 1))
        ou_ref[k] = u_star
        ov_ref[k] = v_star
        return (pc, pe, pw, pn_, ps_, flux_t, flux_s, tu + h * u_star, tv + h * v_star, height + h * mc)

    unroll = 4 if K % 4 == 0 else 1

    def group(g, carry):
        for i in range(unroll):
            carry = level(g * unroll + i, carry)
        return carry

    carry = lax.fori_loop(0, K // unroll, group, (zero,) * 10)
    op_ref[0] = carry[9]
    op_ref[1] = sea_ref[...].astype(F32) * eta_ref[...]
    op_ref[2] = drive_ref[...]
    op_ref[3] = carry[7]
    op_ref[4] = carry[8]

    to_east.wait_send()
    to_west.wait_send()

    @pl.when(not_south)
    def _():
        for out in (SLOT_S, SLOT_SE, SLOT_SW):
            edge(spk, SLOT_N, p, q, out).wait_send()

    edge(npk, SLOT_N, p, q, SLOT_N).wait_send()

    @pl.when(ne_remote)
    def _():
        edge(npk, SLOT_NE, p, q, SLOT_NE).wait_send()

    @pl.when(nw_remote)
    def _():
        edge(npk, SLOT_NW, p, q, SLOT_NW).wait_send()


def surface_solve(load, n_lon, n_lat, K, NI, NJ, cells):
    tiles = range(n_lat)
    lines = range(NI)
    lane = iota((n_lon, NJ), 1)

    def every(fn, *arrays):
        return [[fn(*(a[b][s] for a in arrays)) for s in lines] for b in tiles]

    def east(x):
        return [x[b][1:] + [pltpu.roll(x[b][0], n_lon - 1, 0)] for b in tiles]

    def west(x):
        return [[pltpu.roll(x[b][NI - 1], 1, 0)] + x[b][:-1] for b in tiles]

    def north(x, sign):
        out = []
        for b in tiles:
            row = []
            for s in lines:
                if b + 1 < n_lat:
                    beyond = pltpu.roll(x[b + 1][s], NJ - 1, 1)
                else:
                    beyond = flip_rows(x[b][NI - 1 - s])
                    beyond = -beyond if sign < 0 else beyond
                row.append(jnp.where(lane == NJ - 1, beyond, pltpu.roll(x[b][s], NJ - 1, 1)))
            out.append(row)
        return out

    def south(x):
        out = []
        for b in tiles:
            row = []
            for s in lines:
                beyond = pltpu.roll(x[b - 1][s], 1, 1) if b > 0 else 0.0
                row.append(jnp.where(lane == 0, beyond, pltpu.roll(x[b][s], 1, 1)))
            out.append(row)
        return out

    height = load(0)
    scale = lambda a, c: jnp.minimum(a, c) * (1.0 / K)
    w_e = every(scale, height, east(height))
    w_w = every(scale, height, west(height))
    w_n = every(scale, height, north(height, 1))
    w_s = every(scale, height, south(height))
    diag = every(lambda a, b, c, d: STORAGE + a + b + c + d, w_e, w_w, w_n, w_s)

    def apply(x):
        return every(
            lambda dg, c, we, e, ww, w, wn, n, ws, s: dg * c - (we * e + ww * w + wn * n + ws * s),
            diag, x, w_e, east(x), w_w, west(x), w_n, north(x, 1), w_s, south(x))

    factors = [[None] * NI for _ in tiles]
    pivots = [[None] * NI for _ in tiles]
    for b in tiles:
        for s in lines:
            pivot = diag[b][s]
            if s > 0:
                pivot = pivot + w_w[b][s] * factors[b][s - 1]
            pivots[b][s] = 1.0 / pivot
            factors[b][s] = -w_e[b][s] * pivots[b][s]

    def precondition(r):
        out = []
        for b in tiles:
            part = []
            for s in lines:
                value = r[b][s]
                if s > 0:
                    value = value + w_w[b][s] * part[s - 1]
                part.append(value * pivots[b][s])
            for s in range(NI - 2, -1, -1):
                part[s] = part[s] - factors[b][s] * part[s + 1]
            out.append(part)
        return out

    x = load(1)
    drive = load(2)
    t_u = load(3)
    t_v = load(4)
    right = every(
        lambda h, d, e, w, n, s: jnp.where(h > 0.0, d - DIVERGENCE * (0.5 * (e - w) + 0.5 * (n - s)), 0.0),
        height, drive, east(t_u), west(t_u), north(t_v, -1), south(t_v))
    residual = every(lambda a, b: a - b, right, apply(x))
    mid = 0.5 * (SPECTRUM_HIGH + SPECTRUM_LOW)
    half = 0.5 * (SPECTRUM_HIGH - SPECTRUM_LOW)
    ratio = mid / half
    direction = every(lambda a: a / mid, precondition(residual))
    rho = 1.0 / ratio
    for step in range(ITERS):
        x = every(lambda a, b: a + b, x, direction)
        residual = every(lambda a, b: a - b, residual, apply(direction))
        if step + 1 < ITERS:
            rho_next = 1.0 / (2.0 * ratio - rho)
            keep, gain = rho_next * rho, 2.0 * rho_next / half
            direction = every(lambda d, z: keep * d + gain * z, direction, precondition(residual))
            rho = rho_next
    squares = every(lambda a: a * a, residual)
    total = functools.reduce(lambda a, b: a + b, [squares[b][s] for b in tiles for s in lines])
    total = jnp.sum(jnp.sum(total, axis=1, keepdims=True), axis=0, keepdims=True)
    rms = jnp.sqrt(total / cells + EPSILON)
    slope_x = every(lambda e, w: 0.5 * (e - w), east(x), west(x))
    slope_y = every(lambda n, s: 0.5 * (n - s), north(x, 1), south(x))
    return x, slope_x, slope_y, rms


def solve_kernel(n_lon, n_lat, g_ref, us_ref, vs_ref, num_ref, sea_ref, ou_ref, ov_ref, ox_ref,
                 orms_ref, held):
    K, NI, NJ = us_ref.shape
    p = lax.axis_index("lon")
    q = lax.axis_index("lat")

    flat = g_ref.reshape(n_lat * n_lon * FIELDS * NI, NJ)

    def load(f):
        return [[flat[pl.ds((b * n_lon * FIELDS + f) * NI + s, n_lon, stride=FIELDS * NI), :]
                 for s in range(NI)] for b in range(n_lat)]

    x, slope_x, slope_y, rms = surface_solve(load, n_lon, n_lat, K, NI, NJ, n_lon * NI * n_lat * NJ)
    for i, field in enumerate((x, slope_x, slope_y)):
        for b in range(n_lat):
            for s in range(NI):
                held[i, b, pl.ds(s, n_lon, stride=NI), :] = field[b][s]
    orms_ref[0] = jnp.max(jnp.broadcast_to(rms, (8, 128)))
    mine = pl.ds(pl.multiple_of(p * NI, NI), NI)
    ox_ref[...] = held[0, q, mine, :]
    su = GRAVITY * held[1, q, mine, :]
    sv = GRAVITY * held[2, q, mine, :]
    depth = (num_ref[...] * sea_ref[...]).astype(F32)
    for k in range(K):
        wet = depth > k + 0.5
        ou_ref[k] = jnp.where(wet, us_ref[k] - su, 0.0)
        ov_ref[k] = jnp.where(wet, vs_ref[k] - sv, 0.0)


def per_device(n_lon, n_lat, temp, salt, u, v, num, sea, thick, eta, drive):
    K, NI, NJ = temp.shape
    vmem = pl.BlockSpec(memory_space=pltpu.VMEM)
    smem = pl.BlockSpec(memory_space=pltpu.SMEM)
    big = jax.ShapeDtypeStruct((K, NI, NJ), F32)
    new_t, new_s, u_star, v_star, packet = pl.pallas_call(
        functools.partial(step_kernel, n_lon, n_lat),
        out_shape=(big, big, big, big, jax.ShapeDtypeStruct((FIELDS, NI, NJ), F32)),
        in_specs=[vmem] * 6 + [smem] + [vmem] * 2,
        out_specs=(vmem,) * 5,
        scratch_shapes=[
            pltpu.VMEM((6 * K + NI, NJ), F32), pltpu.VMEM((6 * K + NI, NJ), F32),
            pltpu.VMEM((2, NI, NJ), F32), pltpu.VMEM((2, NI, NJ), F32),
            pltpu.VMEM((6 * K + NI, NJ), F32), pltpu.VMEM((6 * K + NI, NJ), F32),
            pltpu.VMEM((6, 2, NI, NJ), F32), pltpu.VMEM((6, K, NJ), F32),
            pltpu.SemaphoreType.DMA((8,)), pltpu.SemaphoreType.DMA((8,)),
        ],
        compiler_params=pltpu.CompilerParams(collective_id=0, has_side_effects=True),
        name="step",
    )(temp, salt, u, v, num, sea, thick, eta, drive)
    gathered = lax.all_gather(packet, ("lat", "lon")).reshape(n_lat, n_lon, FIELDS, NI, NJ)
    new_u, new_v, surface, rms = pl.pallas_call(
        functools.partial(solve_kernel, n_lon, n_lat),
        out_shape=(big, big, jax.ShapeDtypeStruct((NI, NJ), F32), jax.ShapeDtypeStruct((1,), F32)),
        in_specs=[vmem] * 5,
        out_specs=(vmem, vmem, vmem, smem),
        scratch_shapes=[pltpu.VMEM((3, n_lat, n_lon * NI, NJ), F32)],
        name="solve",
    )(gathered, u_star, v_star, num, sea)
    return new_t, new_s, new_u, new_v, surface, rms.reshape(())


def solution(mesh):
    n_lon, n_lat = mesh.shape["lon"], mesh.shape["lat"]
    spec3 = P(None, "lon", "lat")
    spec2 = P("lon", "lat")
    return jax.shard_map(
        functools.partial(per_device, n_lon, n_lat),
        mesh=mesh,
        in_specs=(spec3, spec3, spec3, spec3, spec2, spec2, P(), spec2, spec2),
        out_specs=(spec3, spec3, spec3, spec3, spec2, P()),
        check_vma=False,
    )
```

```python
import functools

import jax
import jax.numpy as jnp
from jax import lax
from jax.experimental import pallas as pl
from jax.experimental.pallas import tpu as pltpu
from jax.sharding import PartitionSpec as P

ITERS = 4
DIFFUSION = 0.15
MIXING = 0.1
EXPANSION = 0.2
CONTRACTION = 0.15
PRESSURE_SCALE = 0.02
CORIOLIS = 0.5
FRICTION = 0.01
DIVERGENCE = 0.3
STORAGE = 0.1
SPECTRUM_LOW = 0.1
SPECTRUM_HIGH = 1.9
GRAVITY = 0.3
EPSILON = 1e-06

MESH = pl.DeviceIdType.MESH
F32 = jnp.float32
SLOT_N, SLOT_NE, SLOT_NW, SLOT_S, SLOT_SE, SLOT_SW = range(6)
SEM_E, SEM_W = 6, 7
EARLY = 3
LATE = 2


def iota(shape, axis):
    return lax.broadcasted_iota(jnp.int32, shape, axis)


def flip_rows(x):
    n = x.shape[0]
    row = iota(x.shape, 0)
    bit = n // 2
    while bit:
        up = pltpu.roll(x, bit, 0)
        down = pltpu.roll(x, n - bit, 0)
        x = up if 2 * bit == n else jnp.where((row & bit) != 0, up, down)
        bit //= 2
    return x


def step_kernel(n_lon, n_lat, t_ref, s_ref, u_ref, v_ref, num_ref, sea_ref, thick_ref, eta_ref,
                drive_ref, ot_ref, os_ref, ou_ref, ov_ref, ox_ref, orms_ref, epk, wpk, npk, spk, slot_e,
                slot_w, slots, rim, early, late, held, send_sem, recv_sem, cast_send, cast_recv):
    K, NI, NJ = t_ref.shape
    p = lax.axis_index("lon")
    q = lax.axis_index("lat")
    east_dev = lax.rem(p + 1, n_lon)
    west_dev = lax.rem(p + n_lon - 1, n_lon)
    at_pole = q == n_lat - 1
    not_pole = q < n_lat - 1
    not_south = q > 0
    mirror = n_lon - 1 - p
    mirror_ne = lax.rem(2 * n_lon - 2 - p, n_lon)
    mirror_nw = lax.rem(2 * n_lon - p, n_lon)
    ne_remote = jnp.logical_or(not_pole, mirror_ne != p)
    nw_remote = jnp.logical_or(not_pole, mirror_nw != p)
    ne_self = jnp.logical_and(at_pole, mirror_ne == p)
    nw_self = jnp.logical_and(at_pole, mirror_nw == p)

    barrier = pltpu.get_barrier_semaphore()

    def greet(lon, lat):
        pl.semaphore_signal(barrier, inc=1, device_id={"lon": lon, "lat": lat}, device_id_type=MESH)

    greet(east_dev, q)
    greet(west_dev, q)

    @pl.when(not_south)
    def _():
        for lon in (p, east_dev, west_dev):
            greet(lon, q - 1)

    @pl.when(not_pole)
    def _():
        for lon in (p, east_dev, west_dev):
            greet(lon, q + 1)

    @pl.when(at_pole)
    def _():
        greet(mirror, q)

    @pl.when(jnp.logical_and(at_pole, mirror_ne != p))
    def _():
        greet(mirror_ne, q)

    @pl.when(jnp.logical_and(at_pole, mirror_nw != p))
    def _():
        greet(mirror_nw, q)

    parity = lax.rem(q, 2)
    partner = q + 1 - 2 * parity
    n_half = n_lon * n_lat // 2
    me_half = (q // 2) * n_lon + p

    def half_peer(r):
        other = lax.rem(me_half + r, n_half)
        return lax.rem(other, n_lon), 2 * (other // n_lon) + parity

    def greet_half(r, carry):
        greet(*half_peer(r))
        return carry

    lax.fori_loop(1, n_half, greet_half, 0)
    greet(p, partner)

    sub = iota((NI, NJ), 0)
    lane = iota((NI, NJ), 1)
    depth = (num_ref[...] * sea_ref[...]).astype(F32)
    height = jnp.zeros((NI, NJ), F32)
    for k in range(K):
        height = height + jnp.where(depth > k + 0.5, thick_ref[k], 0.0)
    early[parity, me_half, 0] = height
    early[parity, me_half, 1] = sea_ref[...].astype(F32) * eta_ref[...]
    early[parity, me_half, 2] = drive_ref[...]

    fields = (t_ref, s_ref, u_ref, v_ref)
    for pk, d1, d2 in ((epk, NI - 1, NI - 2), (wpk, 0, 1)):
        for f, ref in enumerate(fields):
            pk[f * K:(f + 1) * K, :] = ref[:, d1, :]
        pk[4 * K:5 * K, :] = u_ref[:, d2, :]
        pk[5 * K:6 * K, :] = v_ref[:, d2, :]
        pk[6 * K:6 * K + NI, :] = jnp.zeros((NI, NJ), F32)
        pk[6 * K:6 * K + 1, :] = depth[d1:d1 + 1, :]
        pk[6 * K + 1:6 * K + 2, :] = depth[d2:d2 + 1, :]

    n0 = jnp.zeros((NI, NJ), F32)
    s0 = jnp.zeros((NI, NJ), F32)
    n1 = jnp.zeros((NI, NJ), F32)
    s1 = jnp.zeros((NI, NJ), F32)

    def put(acc, x, source, target):
        moved = pltpu.roll(x, (target - source) % NJ, 1) if source != target else x
        return jnp.where(lane == target, moved, acc)

    for f, ref in enumerate(fields):
        for k in range(K):
            x = ref[k]
            target = f * K + k
            n0 = put(n0, x, NJ - 1, target)
            s0 = put(s0, x, 0, target)
            if f >= 2:
                n1 = put(n1, x, NJ - 2, target)
                s1 = put(s1, x, 1, target)
    n1 = put(put(n1, depth, NJ - 1, 0), depth, NJ - 2, 1)
    s1 = put(put(s1, depth, 0, 0), depth, 1, 1)
    npk[0] = n0
    npk[1] = n1
    spk[0] = s0
    spk[1] = s1

    peers = (3 + n_half + 2 * not_pole.astype(jnp.int32) + 3 * not_south.astype(jnp.int32)
             + at_pole.astype(jnp.int32) * ((mirror_ne != p).astype(jnp.int32) + (mirror_nw != p).astype(jnp.int32)))
    pl.semaphore_wait(barrier, peers)

    def copy(src, dst, lon, lat, out, into):
        return pltpu.make_async_remote_copy(
            src_ref=src, dst_ref=dst, send_sem=send_sem.at[out], recv_sem=recv_sem.at[into],
            device_id={"lon": lon, "lat": lat}, device_id_type=MESH)

    def edge(src, slot, lon, lat, out):
        return copy(src, slots.at[slot], lon, lat, out, slot)

    to_east = copy(epk, slot_w, east_dev, q, SEM_E, SEM_W)
    to_west = copy(wpk, slot_e, west_dev, q, SEM_W, SEM_E)
    to_east.start()
    to_west.start()

    @pl.when(not_south)
    def _():
        edge(spk, SLOT_N, p, q - 1, SLOT_S).start()
        edge(spk, SLOT_NW, east_dev, q - 1, SLOT_SE).start()
        edge(spk, SLOT_NE, west_dev, q - 1, SLOT_SW).start()

    @pl.when(not_pole)
    def _():
        edge(npk, SLOT_S, p, q + 1, SLOT_N).start()
        edge(npk, SLOT_SW, east_dev, q + 1, SLOT_NE).start()
        edge(npk, SLOT_SE, west_dev, q + 1, SLOT_NW).start()

    @pl.when(at_pole)
    def _():
        edge(npk, SLOT_N, mirror, q, SLOT_N).start()

    @pl.when(jnp.logical_and(at_pole, mirror_ne != p))
    def _():
        edge(npk, SLOT_NE, mirror_ne, q, SLOT_NE).start()

    @pl.when(jnp.logical_and(at_pole, mirror_nw != p))
    def _():
        edge(npk, SLOT_NW, mirror_nw, q, SLOT_NW).start()

    def cast(buf, which):
        def send(r, carry):
            lon, lat = half_peer(r)
            mine = buf.at[parity, me_half]
            pltpu.make_async_remote_copy(
                src_ref=mine, dst_ref=mine, send_sem=cast_send.at[which], recv_sem=cast_recv.at[which],
                device_id={"lon": lon, "lat": lat}, device_id_type=MESH).start()
            return carry

        lax.fori_loop(1, n_half, send, 0)

    def cast_wait(buf, sem):
        rest = buf.at[parity, pl.ds(0, n_half - 1)]
        pltpu.make_async_copy(rest, rest, sem).wait()

    def hand_over(buf, which):
        return pltpu.make_async_remote_copy(
            src_ref=buf.at[parity], dst_ref=buf.at[parity], send_sem=cast_send.at[which],
            recv_sem=cast_recv.at[which], device_id={"lon": p, "lat": partner}, device_id_type=MESH)

    cast(early, 0)

    edge(npk, SLOT_N, p, q, SLOT_N).wait_recv()

    @pl.when(ne_remote)
    def _():
        edge(npk, SLOT_NE, p, q, SLOT_NE).wait_recv()

    @pl.when(nw_remote)
    def _():
        edge(npk, SLOT_NW, p, q, SLOT_NW).wait_recv()

    @pl.when(not_south)
    def _():
        for slot in (SLOT_S, SLOT_SE, SLOT_SW):
            edge(spk, slot, p, q, slot).wait_recv()

    sign = jnp.where(lane >= 2 * K, -1.0, 1.0).astype(F32)

    def northern(slot, own):
        out = []
        for i in range(2):
            x = slots[slot, i]
            if own is not None:
                x = jnp.where(own, npk[i], x)
            out.append(jnp.where(at_pole, flip_rows(x) * sign, x))
        return out

    def southern(slot):
        return [jnp.where(not_south, slots[slot, i], 0.0) for i in range(2)]

    pn0, pn1 = northern(SLOT_N, None)
    pne0, pne1 = northern(SLOT_NE, ne_self)
    pnw0, pnw1 = northern(SLOT_NW, nw_self)
    ps0, ps1 = southern(SLOT_S)
    pse0, pse1 = southern(SLOT_SE)
    psw0, psw1 = southern(SLOT_SW)

    def shift_e(x, row):
        return jnp.where(sub == NI - 1, row, pltpu.roll(x, NI - 1, 0))

    def shift_w(x, row):
        return jnp.where(sub == 0, row, pltpu.roll(x, 1, 0))

    level_l = (lane - K * (lane // K)).astype(F32) + 0.5

    def wet_l(d):
        return jnp.where(level_l < d, 1.0, 0.0)

    def spread(x, i):
        return jnp.broadcast_to(x[:, i:i + 1], (NI, NJ))

    def packed_lap(c0, c1, e0, e1, w0, w1, own, own_depth):
        d = spread(c1, 0)
        de = shift_e(d, jnp.broadcast_to(e1[0:1, 0:1], (NI, NJ)))
        dw = shift_w(d, jnp.broadcast_to(w1[NI - 1:NI, 0:1], (NI, NJ)))
        xe = shift_e(c0, jnp.broadcast_to(e0[0:1, :], (NI, NJ)))
        xw = shift_w(c0, jnp.broadcast_to(w0[NI - 1:NI, :], (NI, NJ)))
        total = wet_l(de) * (xe - c0) + wet_l(dw) * (xw - c0)
        total = total + wet_l(spread(c1, 1)) * (c1 - c0) + wet_l(own_depth) * (own - c0)
        return wet_l(d) * total

    lap_n = packed_lap(pn0, pn1, pne0, pne1, pnw0, pnw1, n0, spread(depth, NJ - 1))
    lap_s = packed_lap(ps0, ps1, pse0, pse1, psw0, psw1, s0, spread(depth, 0))
    rim[4, 0:NI, :] = lap_n
    rim[5, 0:NI, :] = lap_s
    rim[4, NI:2 * NI, :] = pn0
    rim[5, NI:2 * NI, :] = ps0

    to_east.wait_recv()
    to_west.wait_recv()

    level_r = iota((K, NJ), 0)
    lane_r = iota((K, NJ), 1)
    level_rf = level_r.astype(F32) + 0.5

    def wet_r(d):
        return jnp.where(level_rf < d, 1.0, 0.0)

    def wide(row):
        return jnp.broadcast_to(row, (K, NJ))

    for side, (slot, pk, d1, cn0, cn1, cs0, cs1) in enumerate((
            (slot_e, epk, NI - 1, pne0[0:1], pne1[0:1], pse0[0:1], pse1[0:1]),
            (slot_w, wpk, 0, pnw0[NI - 1:], pnw1[NI - 1:], psw0[NI - 1:], psw1[NI - 1:]))):
        d = wide(slot[6 * K:6 * K + 1, :])
        far = wet_r(wide(slot[6 * K + 1:6 * K + 2, :]))
        own = wet_r(wide(depth[d1:d1 + 1, :]))
        dn = jnp.where(lane_r == NJ - 1, jnp.broadcast_to(cn1[:, 0:1], (K, NJ)), pltpu.roll(d, NJ - 1, 1))
        ds = jnp.where(lane_r == 0, jnp.broadcast_to(cs1[:, 0:1], (K, NJ)), pltpu.roll(d, 1, 1))
        mid, mn, ms = wet_r(d), wet_r(dn), wet_r(ds)
        for i in range(2):
            f = 2 + i
            x = slot[f * K:(f + 1) * K, :]
            pick = lane_r == level_r + f * K
            cn = jnp.sum(jnp.where(pick, wide(cn0), 0.0), axis=1, keepdims=True)
            cs = jnp.sum(jnp.where(pick, wide(cs0), 0.0), axis=1, keepdims=True)
            xn = jnp.where(lane_r == NJ - 1, jnp.broadcast_to(cn, (K, NJ)), pltpu.roll(x, NJ - 1, 1))
            xs = jnp.where(lane_r == 0, jnp.broadcast_to(cs, (K, NJ)), pltpu.roll(x, 1, 1))
            total = far * (slot[(4 + i) * K:(5 + i) * K, :] - x) + own * (pk[f * K:(f + 1) * K, :] - x)
            total = total + mn * (xn - x) + ms * (xs - x)
            rim[2 * side + i] = mid * total

    def shift_n(x, packed, source):
        return jnp.where(lane == NJ - 1, pltpu.roll(packed, NJ - 1 - source, 1), pltpu.roll(x, NJ - 1, 1))

    def shift_s(x, packed, source):
        return jnp.where(lane == 0, pltpu.roll(packed, lax.rem(NJ - source, NJ), 1), pltpu.roll(x, 1, 1))

    depth_e = shift_e(depth, slot_e[6 * K:6 * K + 1, :])
    depth_w = shift_w(depth, slot_w[6 * K:6 * K + 1, :])
    depth_n = shift_n(depth, pn1, 0)
    depth_s = jnp.where(lane == 0, ps1, pltpu.roll(depth, 1, 1))
    both_e = jnp.minimum(depth, depth_e)
    both_w = jnp.minimum(depth, depth_w)
    both_n = jnp.minimum(depth, depth_n)
    both_s = jnp.minimum(depth, depth_s)
    lat_index = (q * NJ + lane).astype(F32)
    coriolis = CORIOLIS * (2.0 * (lat_index + 0.5) / (n_lat * NJ) - 1.0)

    zero = jnp.zeros((NI, NJ), F32)

    def level(k, carry):
        pc, pe, pw, pn_, ps_, flux_t, flux_s, tu, tv = carry
        kf = lax.convert_element_type(k, F32) + 0.5
        h = thick_ref[k]
        nxt = jnp.minimum(k + 1, K - 1)
        h_next = thick_ref[nxt]
        hv = jnp.full((NI, NJ), h, F32)
        inv_space = 1.0 / (0.5 * (hv + h_next))
        inv_h = MIXING / hv

        def wet(d):
            return jnp.where(d > kf, 1.0, 0.0)

        mc = wet(depth)
        me, mw, mn, ms = wet(both_e), wet(both_w), wet(both_n), wet(both_s)
        below = jnp.where(jnp.logical_and(depth > kf + 1.0, k < K - 1), inv_space, 0.0)
        pn0v = rim[4, NI:2 * NI, :]
        ps0v = rim[5, NI:2 * NI, :]
        lapn = rim[4, 0:NI, :]
        laps = rim[5, 0:NI, :]

        def around(ref, f):
            x = ref[k]
            row = pl.ds(f * K + k, 1)
            return (x, shift_e(x, slot_e[row, :]), shift_w(x, slot_w[row, :]),
                    shift_n(x, pn0v, f * K + k), shift_s(x, ps0v, f * K + k))

        t = around(t_ref, 0)
        s = around(s_ref, 1)
        u = around(u_ref, 2)
        v = around(v_ref, 3)
        ae = 0.25 * me * (u[0] + u[1])
        aw = 0.25 * mw * (u[0] + u[2])
        an = 0.25 * mn * (v[0] + v[3])
        as_ = 0.25 * ms * (v[0] + v[4])
        ge, gw, gn, gs = DIFFUSION * me, DIFFUSION * mw, DIFFUSION * mn, DIFFUSION * ms

        def tracer(x, ref, flux_above):
            c, e, w, n, so = x
            total = aw * (w + c) - gw * (c - w) - ae * (c + e) + ge * (e - c)
            total = total + as_ * (so + c) - gs * (c - so) - an * (c + n) + gn * (n - c)
            flux = below * (ref[nxt] - c)
            return mc * (c + total + inv_h * (flux - flux_above)), flux

        new_t, flux_t = tracer(t, t_ref, flux_t)
        new_s, flux_s = tracer(s, s_ref, flux_s)
        ot_ref[k] = new_t
        os_ref[k] = new_s
        pressures = []
        for i, (acc, d) in enumerate(((pc, depth), (pe, depth_e), (pw, depth_w), (pn_, depth_n), (ps_, depth_s))):
            density = CONTRACTION * s[i] - EXPANSION * t[i]
            pressures.append(acc + jnp.where(d > kf, density * h, 0.0))
        pc, pe, pw, pn_, ps_ = pressures
        grad_x = 0.5 * (me * (pe - pc) + mw * (pc - pw))
        grad_y = 0.5 * (mn * (pn_ - pc) + ms * (pc - ps_))

        def biharmonic(x, i):
            c, e, w, n, so = x
            lap = me * (e - c) + mw * (w - c) + mn * (n - c) + ms * (so - c)
            row = pl.ds(k, 1)
            le = shift_e(lap, rim[i, row, :])
            lw = shift_w(lap, rim[2 + i, row, :])
            source = (2 + i) * K + k
            ln = shift_n(lap, lapn, source)
            ls = shift_s(lap, laps, source)
            return me * (le - lap) + mw * (lw - lap) + mn * (ln - lap) + ms * (ls - lap)

        u_star = mc * (u[0] + coriolis * v[0] - PRESSURE_SCALE * grad_x - FRICTION * biharmonic(u, 0))
        v_star = mc * (v[0] - coriolis * u[0] - PRESSURE_SCALE * grad_y - FRICTION * biharmonic(v, 1))
        ou_ref[k] = u_star
        ov_ref[k] = v_star
        return (pc, pe, pw, pn_, ps_, flux_t, flux_s, tu + h * u_star, tv + h * v_star)

    unroll = 4 if K % 4 == 0 else 1

    def group(g, carry):
        for i in range(unroll):
            carry = level(g * unroll + i, carry)
        return carry

    carry = lax.fori_loop(0, K // unroll, group, (zero,) * 9)
    late[parity, me_half, 0] = carry[7]
    late[parity, me_half, 1] = carry[8]
    cast(late, 1)

    cast_wait(early, cast_recv.at[0])
    early_over = hand_over(early, 2)
    early_over.start()
    early_over.wait_recv()

    def loader(buf, count):
        flat = buf.reshape(2 * n_half * count * NI, NJ)

        def load(f):
            return [[flat[pl.ds((((b % 2) * n_half + (b // 2) * n_lon) * count + f) * NI + s, n_lon,
                                stride=count * NI), :] for s in range(NI)] for b in range(n_lat)]

        return load

    def late_loader():
        cast_wait(late, cast_recv.at[1])
        late_over = hand_over(late, 3)
        late_over.start()
        late_over.wait_recv()
        return loader(late, LATE)

    x, slope_x, slope_y, rms = surface_solve(loader(early, EARLY), late_loader, n_lon, n_lat, K, NI, NJ,
                                             n_lon * NI * n_lat * NJ)
    for i, field in enumerate((x, slope_x, slope_y)):
        for b in range(n_lat):
            for s in range(NI):
                held[i, b, pl.ds(s, n_lon, stride=NI), :] = field[b][s]
    orms_ref[0] = jnp.max(jnp.broadcast_to(rms, (8, 128)))
    block = pl.ds(pl.multiple_of(p * NI, NI), NI)
    ox_ref[...] = held[0, q, block, :]
    su = GRAVITY * held[1, q, block, :]
    sv = GRAVITY * held[2, q, block, :]
    for k in range(K):
        wet = depth > k + 0.5
        ou_ref[k] = jnp.where(wet, ou_ref[k] - su, 0.0)
        ov_ref[k] = jnp.where(wet, ov_ref[k] - sv, 0.0)

    cast_wait(early, cast_send.at[0])
    cast_wait(late, cast_send.at[1])
    early_over.wait_send()
    hand_over(late, 3).wait_send()

    to_east.wait_send()
    to_west.wait_send()

    @pl.when(not_south)
    def _():
        for out in (SLOT_S, SLOT_SE, SLOT_SW):
            edge(spk, SLOT_N, p, q, out).wait_send()

    edge(npk, SLOT_N, p, q, SLOT_N).wait_send()

    @pl.when(ne_remote)
    def _():
        edge(npk, SLOT_NE, p, q, SLOT_NE).wait_send()

    @pl.when(nw_remote)
    def _():
        edge(npk, SLOT_NW, p, q, SLOT_NW).wait_send()


def surface_solve(load, load_late, n_lon, n_lat, K, NI, NJ, cells):
    tiles = range(n_lat)
    lines = range(NI)
    lane = iota((n_lon, NJ), 1)

    def every(fn, *arrays):
        return [[fn(*(a[b][s] for a in arrays)) for s in lines] for b in tiles]

    def east(x):
        return [x[b][1:] + [pltpu.roll(x[b][0], n_lon - 1, 0)] for b in tiles]

    def west(x):
        return [[pltpu.roll(x[b][NI - 1], 1, 0)] + x[b][:-1] for b in tiles]

    def north(x, sign):
        out = []
        for b in tiles:
            row = []
            for s in lines:
                if b + 1 < n_lat:
                    beyond = pltpu.roll(x[b + 1][s], NJ - 1, 1)
                else:
                    beyond = flip_rows(x[b][NI - 1 - s])
                    beyond = -beyond if sign < 0 else beyond
                row.append(jnp.where(lane == NJ - 1, beyond, pltpu.roll(x[b][s], NJ - 1, 1)))
            out.append(row)
        return out

    def south(x):
        out = []
        for b in tiles:
            row = []
            for s in lines:
                beyond = pltpu.roll(x[b - 1][s], 1, 1) if b > 0 else 0.0
                row.append(jnp.where(lane == 0, beyond, pltpu.roll(x[b][s], 1, 1)))
            out.append(row)
        return out

    height = load(0)
    scale = lambda a, c: jnp.minimum(a, c) * (1.0 / K)
    w_e = every(scale, height, east(height))
    w_w = every(scale, height, west(height))
    w_n = every(scale, height, north(height, 1))
    w_s = every(scale, height, south(height))
    diag = every(lambda a, b, c, d: STORAGE + a + b + c + d, w_e, w_w, w_n, w_s)

    def apply(x):
        return every(
            lambda dg, c, we, e, ww, w, wn, n, ws, s: dg * c - (we * e + ww * w + wn * n + ws * s),
            diag, x, w_e, east(x), w_w, west(x), w_n, north(x, 1), w_s, south(x))

    factors = [[None] * NI for _ in tiles]
    pivots = [[None] * NI for _ in tiles]
    for b in tiles:
        for s in lines:
            pivot = diag[b][s]
            if s > 0:
                pivot = pivot + w_w[b][s] * factors[b][s - 1]
            pivots[b][s] = 1.0 / pivot
            factors[b][s] = -w_e[b][s] * pivots[b][s]

    def precondition(r):
        out = []
        for b in tiles:
            part = []
            for s in lines:
                value = r[b][s]
                if s > 0:
                    value = value + w_w[b][s] * part[s - 1]
                part.append(value * pivots[b][s])
            for s in range(NI - 2, -1, -1):
                part[s] = part[s] - factors[b][s] * part[s + 1]
            out.append(part)
        return out

    x = load(1)
    drive = load(2)
    start = every(lambda h, d, a: jnp.where(h > 0.0, d, 0.0) - a, height, drive, apply(x))
    load = load_late()
    t_u = load(0)
    t_v = load(1)
    residual = every(
        lambda h, d, e, w, n, s: d - jnp.where(h > 0.0, 0.5 * DIVERGENCE * ((e - w) + (n - s)), 0.0),
        height, start, east(t_u), west(t_u), north(t_v, -1), south(t_v))
    mid = 0.5 * (SPECTRUM_HIGH + SPECTRUM_LOW)
    half = 0.5 * (SPECTRUM_HIGH - SPECTRUM_LOW)
    ratio = mid / half
    direction = every(lambda a: a / mid, precondition(residual))
    rho = 1.0 / ratio
    for step in range(ITERS):
        x = every(lambda a, b: a + b, x, direction)
        residual = every(lambda a, b: a - b, residual, apply(direction))
        if step + 1 < ITERS:
            rho_next = 1.0 / (2.0 * ratio - rho)
            keep, gain = rho_next * rho, 2.0 * rho_next / half
            direction = every(lambda d, z: keep * d + gain * z, direction, precondition(residual))
            rho = rho_next
    squares = every(lambda a: a * a, residual)
    total = functools.reduce(lambda a, b: a + b, [squares[b][s] for b in tiles for s in lines])
    total = jnp.sum(jnp.sum(total, axis=1, keepdims=True), axis=0, keepdims=True)
    rms = jnp.sqrt(total / cells + EPSILON)
    slope_x = every(lambda e, w: 0.5 * (e - w), east(x), west(x))
    slope_y = every(lambda n, s: 0.5 * (n - s), north(x, 1), south(x))
    return x, slope_x, slope_y, rms


def per_device(n_lon, n_lat, temp, salt, u, v, num, sea, thick, eta, drive):
    K, NI, NJ = temp.shape
    vmem = pl.BlockSpec(memory_space=pltpu.VMEM)
    smem = pl.BlockSpec(memory_space=pltpu.SMEM)
    big = jax.ShapeDtypeStruct((K, NI, NJ), F32)
    n_half = n_lon * n_lat // 2
    row_scratch = pltpu.VMEM((6 * K + NI, NJ), F32)
    new_t, new_s, new_u, new_v, surface, rms = pl.pallas_call(
        functools.partial(step_kernel, n_lon, n_lat),
        out_shape=(big, big, big, big, jax.ShapeDtypeStruct((NI, NJ), F32), jax.ShapeDtypeStruct((1,), F32)),
        in_specs=[vmem] * 6 + [smem] + [vmem] * 2,
        out_specs=(vmem,) * 5 + (smem,),
        scratch_shapes=[
            row_scratch, row_scratch,
            pltpu.VMEM((2, NI, NJ), F32), pltpu.VMEM((2, NI, NJ), F32),
            row_scratch, row_scratch,
            pltpu.VMEM((6, 2, NI, NJ), F32), pltpu.VMEM((6, K, NJ), F32),
            pltpu.VMEM((2, n_half, EARLY, NI, NJ), F32), pltpu.VMEM((2, n_half, LATE, NI, NJ), F32),
            pltpu.VMEM((3, n_lat, n_lon * NI, NJ), F32),
            pltpu.SemaphoreType.DMA((8,)), pltpu.SemaphoreType.DMA((8,)),
            pltpu.SemaphoreType.DMA((4,)), pltpu.SemaphoreType.DMA((4,)),
        ],
        compiler_params=pltpu.CompilerParams(collective_id=0, has_side_effects=True),
        name="step",
    )(temp, salt, u, v, num, sea, thick, eta, drive)
    return new_t, new_s, new_u, new_v, surface, rms.reshape(())


def solution(mesh):
    n_lon, n_lat = mesh.shape["lon"], mesh.shape["lat"]
    spec3 = P(None, "lon", "lat")
    spec2 = P("lon", "lat")
    return jax.shard_map(
        functools.partial(per_device, n_lon, n_lat),
        mesh=mesh,
        in_specs=(spec3, spec3, spec3, spec3, spec2, spec2, P(), spec2, spec2),
        out_specs=(spec3, spec3, spec3, spec3, spec2, P()),
        check_vma=False,
    )
```

```python
import functools

import jax
import jax.numpy as jnp
from jax import lax
from jax.experimental import pallas as pl
from jax.experimental.pallas import tpu as pltpu
from jax.sharding import PartitionSpec as P

ITERS = 4
DIFFUSION = 0.15
MIXING = 0.1
EXPANSION = 0.2
CONTRACTION = 0.15
PRESSURE_SCALE = 0.02
CORIOLIS = 0.5
FRICTION = 0.01
DIVERGENCE = 0.3
STORAGE = 0.1
SPECTRUM_LOW = 0.1
SPECTRUM_HIGH = 1.9
GRAVITY = 0.3
EPSILON = 1e-06

MESH = pl.DeviceIdType.MESH
F32 = jnp.float32
SLOT_N, SLOT_NE, SLOT_NW, SLOT_S, SLOT_SE, SLOT_SW = range(6)
SEM_E, SEM_W = 6, 7
EARLY = 3
LATE = 2


def iota(shape, axis):
    return lax.broadcasted_iota(jnp.int32, shape, axis)


def flip_rows(x):
    n = x.shape[0]
    row = iota(x.shape, 0)
    bit = n // 2
    while bit:
        up = pltpu.roll(x, bit, 0)
        down = pltpu.roll(x, n - bit, 0)
        x = up if 2 * bit == n else jnp.where((row & bit) != 0, up, down)
        bit //= 2
    return x


def step_kernel(n_lon, n_lat, KC, *refs):
    sources, refs = refs[:9], refs[9:]
    ot_ref, os_ref, ou_ref, ov_ref, ox_ref, orms_ref = refs[:6]
    inputs, refs = refs[6:15], refs[15:]
    t_ref, s_ref, u_ref, v_ref, num_ref, sea_ref, thick_ref, eta_ref, drive_ref = inputs
    (epk, wpk, ebase, wbase, npk, spk, slot_e, slot_w, base_e, base_w, slots, rim, early, late, held,
     load_sem, send_sem, recv_sem, side_send, side_recv, cast_send, cast_recv) = refs
    K, NI, NJ = t_ref.shape
    NC = K // KC
    loads = [pltpu.make_async_copy(src, dst, load_sem.at[i]) for i, (src, dst) in enumerate(zip(sources, inputs))]
    for load in loads[4:] + loads[:4]:
        load.start()
    p = lax.axis_index("lon")
    q = lax.axis_index("lat")
    east_dev = lax.rem(p + 1, n_lon)
    west_dev = lax.rem(p + n_lon - 1, n_lon)
    at_pole = q == n_lat - 1
    not_pole = q < n_lat - 1
    not_south = q > 0
    mirror = n_lon - 1 - p
    mirror_ne = lax.rem(2 * n_lon - 2 - p, n_lon)
    mirror_nw = lax.rem(2 * n_lon - p, n_lon)
    ne_remote = jnp.logical_or(not_pole, mirror_ne != p)
    nw_remote = jnp.logical_or(not_pole, mirror_nw != p)
    ne_self = jnp.logical_and(at_pole, mirror_ne == p)
    nw_self = jnp.logical_and(at_pole, mirror_nw == p)

    barrier = pltpu.get_barrier_semaphore()

    def greet(lon, lat):
        pl.semaphore_signal(barrier, inc=1, device_id={"lon": lon, "lat": lat}, device_id_type=MESH)

    greet(east_dev, q)
    greet(west_dev, q)

    @pl.when(not_south)
    def _():
        for lon in (p, east_dev, west_dev):
            greet(lon, q - 1)

    @pl.when(not_pole)
    def _():
        for lon in (p, east_dev, west_dev):
            greet(lon, q + 1)

    @pl.when(at_pole)
    def _():
        greet(mirror, q)

    @pl.when(jnp.logical_and(at_pole, mirror_ne != p))
    def _():
        greet(mirror_ne, q)

    @pl.when(jnp.logical_and(at_pole, mirror_nw != p))
    def _():
        greet(mirror_nw, q)

    parity = lax.rem(q, 2)
    partner = q + 1 - 2 * parity
    n_half = n_lon * n_lat // 2
    me_half = (q // 2) * n_lon + p

    def half_peer(r):
        other = lax.rem(me_half + r, n_half)
        return lax.rem(other, n_lon), 2 * (other // n_lon) + parity

    def greet_half(r, carry):
        greet(*half_peer(r))
        return carry

    lax.fori_loop(1, n_half, greet_half, 0)
    greet(p, partner)

    for load in loads:
        load.wait()
    sub = iota((NI, NJ), 0)
    lane = iota((NI, NJ), 1)
    depth = (num_ref[...] * sea_ref[...]).astype(F32)
    height = jnp.zeros((NI, NJ), F32)
    for k in range(K):
        height = height + jnp.where(depth > k + 0.5, thick_ref[k], 0.0)
    early[parity, me_half, 0] = height
    early[parity, me_half, 1] = sea_ref[...].astype(F32) * eta_ref[...]
    early[parity, me_half, 2] = drive_ref[...]

    fields = (t_ref, s_ref, u_ref, v_ref)
    for pk, base, d1, d2 in ((epk, ebase, NI - 1, NI - 2), (wpk, wbase, 0, 1)):
        for c in range(NC):
            levels = slice(c * KC, (c + 1) * KC)
            for f, (ref, d) in enumerate(((t_ref, d1), (s_ref, d1), (u_ref, d1), (v_ref, d1), (u_ref, d2), (v_ref, d2))):
                pk[c, f * KC:(f + 1) * KC, :] = ref[levels, d, :]
        base[...] = jnp.where(sub == 0, depth[d1:d1 + 1, :], depth[d2:d2 + 1, :])

    n0 = jnp.zeros((NI, NJ), F32)
    s0 = jnp.zeros((NI, NJ), F32)
    n1 = jnp.zeros((NI, NJ), F32)
    s1 = jnp.zeros((NI, NJ), F32)

    def put(acc, x, source, target):
        moved = pltpu.roll(x, (target - source) % NJ, 1) if source != target else x
        return jnp.where(lane == target, moved, acc)

    for f, ref in enumerate(fields):
        for k in range(K):
            x = ref[k]
            target = f * K + k
            n0 = put(n0, x, NJ - 1, target)
            s0 = put(s0, x, 0, target)
            if f >= 2:
                n1 = put(n1, x, NJ - 2, target)
                s1 = put(s1, x, 1, target)
    n1 = put(put(n1, depth, NJ - 1, 0), depth, NJ - 2, 1)
    s1 = put(put(s1, depth, 0, 0), depth, 1, 1)
    npk[0] = n0
    npk[1] = n1
    spk[0] = s0
    spk[1] = s1

    peers = (3 + n_half + 2 * not_pole.astype(jnp.int32) + 3 * not_south.astype(jnp.int32)
             + at_pole.astype(jnp.int32) * ((mirror_ne != p).astype(jnp.int32) + (mirror_nw != p).astype(jnp.int32)))
    pl.semaphore_wait(barrier, peers)

    def copy(src, dst, lon, lat, out, into):
        return pltpu.make_async_remote_copy(
            src_ref=src, dst_ref=dst, send_sem=out, recv_sem=into,
            device_id={"lon": lon, "lat": lat}, device_id_type=MESH)

    def edge(src, slot, lon, lat, out):
        return copy(src, slots.at[slot], lon, lat, send_sem.at[out], recv_sem.at[slot])

    def side_east(c):
        return copy(epk.at[c], slot_w.at[c], east_dev, q, side_send.at[0, c], side_recv.at[0, c])

    def side_west(c):
        return copy(wpk.at[c], slot_e.at[c], west_dev, q, side_send.at[1, c], side_recv.at[1, c])

    base_east = copy(ebase, base_w, east_dev, q, send_sem.at[SEM_E], recv_sem.at[SEM_W])
    base_west = copy(wbase, base_e, west_dev, q, send_sem.at[SEM_W], recv_sem.at[SEM_E])
    base_east.start()
    base_west.start()
    side_east(0).start()
    side_west(0).start()

    @pl.when(not_south)
    def _():
        edge(spk, SLOT_N, p, q - 1, SLOT_S).start()
        edge(spk, SLOT_NW, east_dev, q - 1, SLOT_SE).start()
        edge(spk, SLOT_NE, west_dev, q - 1, SLOT_SW).start()

    @pl.when(not_pole)
    def _():
        edge(npk, SLOT_S, p, q + 1, SLOT_N).start()
        edge(npk, SLOT_SW, east_dev, q + 1, SLOT_NE).start()
        edge(npk, SLOT_SE, west_dev, q + 1, SLOT_NW).start()

    @pl.when(at_pole)
    def _():
        edge(npk, SLOT_N, mirror, q, SLOT_N).start()

    @pl.when(jnp.logical_and(at_pole, mirror_ne != p))
    def _():
        edge(npk, SLOT_NE, mirror_ne, q, SLOT_NE).start()

    @pl.when(jnp.logical_and(at_pole, mirror_nw != p))
    def _():
        edge(npk, SLOT_NW, mirror_nw, q, SLOT_NW).start()

    def cast(buf, which):
        def send(r, carry):
            lon, lat = half_peer(r)
            mine = buf.at[parity, me_half]
            pltpu.make_async_remote_copy(
                src_ref=mine, dst_ref=mine, send_sem=cast_send.at[which], recv_sem=cast_recv.at[which],
                device_id={"lon": lon, "lat": lat}, device_id_type=MESH).start()
            return carry

        lax.fori_loop(1, n_half, send, 0)

    def cast_wait(buf, sem):
        rest = buf.at[parity, pl.ds(0, n_half - 1)]
        pltpu.make_async_copy(rest, rest, sem).wait()

    def hand_over(buf, which):
        return pltpu.make_async_remote_copy(
            src_ref=buf.at[parity], dst_ref=buf.at[parity], send_sem=cast_send.at[which],
            recv_sem=cast_recv.at[which], device_id={"lon": p, "lat": partner}, device_id_type=MESH)

    for c in range(1, NC):
        side_east(c).start()
        side_west(c).start()
    cast(early, 0)

    edge(npk, SLOT_N, p, q, SLOT_N).wait_recv()

    @pl.when(ne_remote)
    def _():
        edge(npk, SLOT_NE, p, q, SLOT_NE).wait_recv()

    @pl.when(nw_remote)
    def _():
        edge(npk, SLOT_NW, p, q, SLOT_NW).wait_recv()

    @pl.when(not_south)
    def _():
        for slot in (SLOT_S, SLOT_SE, SLOT_SW):
            edge(spk, slot, p, q, slot).wait_recv()

    sign = jnp.where(lane >= 2 * K, -1.0, 1.0).astype(F32)

    def northern(slot, own):
        out = []
        for i in range(2):
            x = slots[slot, i]
            if own is not None:
                x = jnp.where(own, npk[i], x)
            out.append(jnp.where(at_pole, flip_rows(x) * sign, x))
        return out

    def southern(slot):
        return [jnp.where(not_south, slots[slot, i], 0.0) for i in range(2)]

    pn0, pn1 = northern(SLOT_N, None)
    pne0, pne1 = northern(SLOT_NE, ne_self)
    pnw0, pnw1 = northern(SLOT_NW, nw_self)
    ps0, ps1 = southern(SLOT_S)
    pse0, pse1 = southern(SLOT_SE)
    psw0, psw1 = southern(SLOT_SW)

    def shift_e(x, row):
        return jnp.where(sub == NI - 1, row, pltpu.roll(x, NI - 1, 0))

    def shift_w(x, row):
        return jnp.where(sub == 0, row, pltpu.roll(x, 1, 0))

    level_l = (lane - K * (lane // K)).astype(F32) + 0.5

    def wet_l(d):
        return jnp.where(level_l < d, 1.0, 0.0)

    def spread(x, i):
        return jnp.broadcast_to(x[:, i:i + 1], (NI, NJ))

    def packed_lap(c0, c1, e0, e1, w0, w1, own, own_depth):
        d = spread(c1, 0)
        de = shift_e(d, jnp.broadcast_to(e1[0:1, 0:1], (NI, NJ)))
        dw = shift_w(d, jnp.broadcast_to(w1[NI - 1:NI, 0:1], (NI, NJ)))
        xe = shift_e(c0, jnp.broadcast_to(e0[0:1, :], (NI, NJ)))
        xw = shift_w(c0, jnp.broadcast_to(w0[NI - 1:NI, :], (NI, NJ)))
        total = wet_l(de) * (xe - c0) + wet_l(dw) * (xw - c0)
        total = total + wet_l(spread(c1, 1)) * (c1 - c0) + wet_l(own_depth) * (own - c0)
        return wet_l(d) * total

    lap_n = packed_lap(pn0, pn1, pne0, pne1, pnw0, pnw1, n0, spread(depth, NJ - 1))
    lap_s = packed_lap(ps0, ps1, pse0, pse1, psw0, psw1, s0, spread(depth, 0))
    rim[4, 0:NI, :] = lap_n
    rim[5, 0:NI, :] = lap_s
    rim[4, NI:2 * NI, :] = pn0
    rim[5, NI:2 * NI, :] = ps0

    base_east.wait_recv()
    base_west.wait_recv()

    row_c = iota((KC, NJ), 0)
    lane_c = iota((KC, NJ), 1)

    def wide(row):
        return jnp.broadcast_to(row, (KC, NJ))

    rim[6, 0:NI, :] = pne0
    rim[6, NI:2 * NI, :] = pse0
    rim[7, 0:NI, :] = pnw0
    rim[7, NI:2 * NI, :] = psw0
    side_depths = []
    for base, d1, cn1, cs1 in ((base_e, NI - 1, pne1[0:1], pse1[0:1]), (base_w, 0, pnw1[NI - 1:], psw1[NI - 1:])):
        d = wide(base[0:1, :])
        dn = jnp.where(lane_c == NJ - 1, jnp.broadcast_to(cn1[:, 0:1], (KC, NJ)), pltpu.roll(d, NJ - 1, 1))
        ds = jnp.where(lane_c == 0, jnp.broadcast_to(cs1[:, 0:1], (KC, NJ)), pltpu.roll(d, 1, 1))
        side_depths.append((d, wide(base[1:2, :]), wide(depth[d1:d1 + 1, :]), dn, ds))

    def side_laps(c):
        level_c = (row_c + c * KC).astype(F32) + 0.5
        for side, (slot, pk, corner) in enumerate(((slot_e, epk, 0), (slot_w, wpk, NI - 1))):
            mid, far, own, mn, ms = [jnp.where(level_c < d, 1.0, 0.0) for d in side_depths[side]]
            cn0 = rim[6 + side, corner:corner + 1, :]
            cs0 = rim[6 + side, NI + corner:NI + corner + 1, :]
            for i in range(2):
                f = 2 + i
                x = slot[c, f * KC:(f + 1) * KC, :]
                pick = lane_c == row_c + (c * KC + f * K)
                cn = jnp.sum(jnp.where(pick, wide(cn0), 0.0), axis=1, keepdims=True)
                cs = jnp.sum(jnp.where(pick, wide(cs0), 0.0), axis=1, keepdims=True)
                xn = jnp.where(lane_c == NJ - 1, jnp.broadcast_to(cn, (KC, NJ)), pltpu.roll(x, NJ - 1, 1))
                xs = jnp.where(lane_c == 0, jnp.broadcast_to(cs, (KC, NJ)), pltpu.roll(x, 1, 1))
                total = far * (slot[c, (4 + i) * KC:(5 + i) * KC, :] - x)
                total = total + own * (pk[c, f * KC:(f + 1) * KC, :] - x) + mn * (xn - x) + ms * (xs - x)
                rim[2 * side + i, 0:KC, :] = mid * total

    def shift_n(x, packed, source):
        return jnp.where(lane == NJ - 1, pltpu.roll(packed, NJ - 1 - source, 1), pltpu.roll(x, NJ - 1, 1))

    def shift_s(x, packed, source):
        return jnp.where(lane == 0, pltpu.roll(packed, lax.rem(NJ - source, NJ), 1), pltpu.roll(x, 1, 1))

    depth_e = shift_e(depth, base_e[0:1, :])
    depth_w = shift_w(depth, base_w[0:1, :])
    depth_n = shift_n(depth, pn1, 0)
    depth_s = jnp.where(lane == 0, ps1, pltpu.roll(depth, 1, 1))
    both_e = jnp.minimum(depth, depth_e)
    both_w = jnp.minimum(depth, depth_w)
    both_n = jnp.minimum(depth, depth_n)
    both_s = jnp.minimum(depth, depth_s)
    lat_index = (q * NJ + lane).astype(F32)
    coriolis = CORIOLIS * (2.0 * (lat_index + 0.5) / (n_lat * NJ) - 1.0)

    zero = jnp.zeros((NI, NJ), F32)

    def level(c, i, carry):
        k = c * KC + i
        inner = i
        pc, pe, pw, pn_, ps_, flux_t, flux_s, tu, tv = carry
        kf = lax.convert_element_type(k, F32) + 0.5
        h = thick_ref[k]
        nxt = jnp.minimum(k + 1, K - 1)
        h_next = thick_ref[nxt]
        hv = jnp.full((NI, NJ), h, F32)
        inv_space = 1.0 / (0.5 * (hv + h_next))
        inv_h = MIXING / hv

        def wet(d):
            return jnp.where(d > kf, 1.0, 0.0)

        mc = wet(depth)
        me, mw, mn, ms = wet(both_e), wet(both_w), wet(both_n), wet(both_s)
        below = jnp.where(jnp.logical_and(depth > kf + 1.0, k < K - 1), inv_space, 0.0)
        pn0v = rim[4, NI:2 * NI, :]
        ps0v = rim[5, NI:2 * NI, :]
        lapn = rim[4, 0:NI, :]
        laps = rim[5, 0:NI, :]

        def around(ref, f):
            x = ref[k]
            row = f * KC + inner
            return (x, shift_e(x, slot_e[c, row:row + 1, :]), shift_w(x, slot_w[c, row:row + 1, :]),
                    shift_n(x, pn0v, f * K + k), shift_s(x, ps0v, f * K + k))

        t = around(t_ref, 0)
        s = around(s_ref, 1)
        u = around(u_ref, 2)
        v = around(v_ref, 3)
        ae = 0.25 * me * (u[0] + u[1])
        aw = 0.25 * mw * (u[0] + u[2])
        an = 0.25 * mn * (v[0] + v[3])
        as_ = 0.25 * ms * (v[0] + v[4])
        ge, gw, gn, gs = DIFFUSION * me, DIFFUSION * mw, DIFFUSION * mn, DIFFUSION * ms

        def tracer(x, ref, flux_above):
            c, e, w, n, so = x
            total = aw * (w + c) - gw * (c - w) - ae * (c + e) + ge * (e - c)
            total = total + as_ * (so + c) - gs * (c - so) - an * (c + n) + gn * (n - c)
            flux = below * (ref[nxt] - c)
            return mc * (c + total + inv_h * (flux - flux_above)), flux

        new_t, flux_t = tracer(t, t_ref, flux_t)
        new_s, flux_s = tracer(s, s_ref, flux_s)
        ot_ref[k] = new_t
        os_ref[k] = new_s
        pressures = []
        for i, (acc, d) in enumerate(((pc, depth), (pe, depth_e), (pw, depth_w), (pn_, depth_n), (ps_, depth_s))):
            density = CONTRACTION * s[i] - EXPANSION * t[i]
            pressures.append(acc + jnp.where(d > kf, density * h, 0.0))
        pc, pe, pw, pn_, ps_ = pressures
        grad_x = 0.5 * (me * (pe - pc) + mw * (pc - pw))
        grad_y = 0.5 * (mn * (pn_ - pc) + ms * (pc - ps_))

        def biharmonic(x, i):
            c, e, w, n, so = x
            lap = me * (e - c) + mw * (w - c) + mn * (n - c) + ms * (so - c)
            le = shift_e(lap, rim[i, inner:inner + 1, :])
            lw = shift_w(lap, rim[2 + i, inner:inner + 1, :])
            source = (2 + i) * K + k
            ln = shift_n(lap, lapn, source)
            ls = shift_s(lap, laps, source)
            return me * (le - lap) + mw * (lw - lap) + mn * (ln - lap) + ms * (ls - lap)

        u_star = mc * (u[0] + coriolis * v[0] - PRESSURE_SCALE * grad_x - FRICTION * biharmonic(u, 0))
        v_star = mc * (v[0] - coriolis * u[0] - PRESSURE_SCALE * grad_y - FRICTION * biharmonic(v, 1))
        ou_ref[k] = u_star
        ov_ref[k] = v_star
        return (pc, pe, pw, pn_, ps_, flux_t, flux_s, tu + h * u_star, tv + h * v_star)

    def chunk(c, carry):
        side_east(c).wait_recv()
        side_west(c).wait_recv()
        side_laps(c)
        for i in range(KC):
            carry = level(c, i, carry)
        return carry

    carry = lax.fori_loop(0, NC, chunk, (zero,) * 9)
    late[parity, me_half, 0] = carry[7]
    late[parity, me_half, 1] = carry[8]
    cast(late, 1)

    cast_wait(early, cast_recv.at[0])
    early_over = hand_over(early, 2)
    early_over.start()
    early_over.wait_recv()

    def loader(buf, count):
        flat = buf.reshape(2 * n_half * count * NI, NJ)

        def load(f):
            return [[flat[pl.ds((((b % 2) * n_half + (b // 2) * n_lon) * count + f) * NI + s, n_lon,
                                stride=count * NI), :] for s in range(NI)] for b in range(n_lat)]

        return load

    def late_loader():
        cast_wait(late, cast_recv.at[1])
        late_over = hand_over(late, 3)
        late_over.start()
        late_over.wait_recv()
        return loader(late, LATE)

    x, slope_x, slope_y, rms = surface_solve(loader(early, EARLY), late_loader, n_lon, n_lat, K, NI, NJ,
                                             n_lon * NI * n_lat * NJ)
    for i, field in enumerate((x, slope_x, slope_y)):
        for b in range(n_lat):
            for s in range(NI):
                held[i, b, pl.ds(s, n_lon, stride=NI), :] = field[b][s]
    orms_ref[0] = jnp.max(jnp.broadcast_to(rms, (8, 128)))
    block = pl.ds(pl.multiple_of(p * NI, NI), NI)
    ox_ref[0] = held[0, q, block, :]
    ox_ref[1] = GRAVITY * held[1, q, block, :]
    ox_ref[2] = GRAVITY * held[2, q, block, :]

    cast_wait(early, cast_send.at[0])
    cast_wait(late, cast_send.at[1])
    early_over.wait_send()
    hand_over(late, 3).wait_send()

    base_east.wait_send()
    base_west.wait_send()
    for c in range(NC):
        side_east(c).wait_send()
        side_west(c).wait_send()

    @pl.when(not_south)
    def _():
        for out in (SLOT_S, SLOT_SE, SLOT_SW):
            edge(spk, SLOT_N, p, q, out).wait_send()

    edge(npk, SLOT_N, p, q, SLOT_N).wait_send()

    @pl.when(ne_remote)
    def _():
        edge(npk, SLOT_NE, p, q, SLOT_NE).wait_send()

    @pl.when(nw_remote)
    def _():
        edge(npk, SLOT_NW, p, q, SLOT_NW).wait_send()


def surface_solve(load, load_late, n_lon, n_lat, K, NI, NJ, cells):
    tiles = range(n_lat)
    lines = range(NI)
    lane = iota((n_lon, NJ), 1)

    def every(fn, *arrays):
        return [[fn(*(a[b][s] for a in arrays)) for s in lines] for b in tiles]

    def east(x):
        return [x[b][1:] + [pltpu.roll(x[b][0], n_lon - 1, 0)] for b in tiles]

    def west(x):
        return [[pltpu.roll(x[b][NI - 1], 1, 0)] + x[b][:-1] for b in tiles]

    def north(x, sign):
        out = []
        for b in tiles:
            row = []
            for s in lines:
                if b + 1 < n_lat:
                    beyond = pltpu.roll(x[b + 1][s], NJ - 1, 1)
                else:
                    beyond = flip_rows(x[b][NI - 1 - s])
                    beyond = -beyond if sign < 0 else beyond
                row.append(jnp.where(lane == NJ - 1, beyond, pltpu.roll(x[b][s], NJ - 1, 1)))
            out.append(row)
        return out

    def south(x):
        out = []
        for b in tiles:
            row = []
            for s in lines:
                beyond = pltpu.roll(x[b - 1][s], 1, 1) if b > 0 else 0.0
                row.append(jnp.where(lane == 0, beyond, pltpu.roll(x[b][s], 1, 1)))
            out.append(row)
        return out

    height = load(0)
    scale = lambda a, c: jnp.minimum(a, c) * (1.0 / K)
    w_e = every(scale, height, east(height))
    w_w = every(scale, height, west(height))
    w_n = every(scale, height, north(height, 1))
    w_s = every(scale, height, south(height))
    diag = every(lambda a, b, c, d: STORAGE + a + b + c + d, w_e, w_w, w_n, w_s)

    def apply(x):
        return every(
            lambda dg, c, we, e, ww, w, wn, n, ws, s: dg * c - (we * e + ww * w + wn * n + ws * s),
            diag, x, w_e, east(x), w_w, west(x), w_n, north(x, 1), w_s, south(x))

    factors = [[None] * NI for _ in tiles]
    pivots = [[None] * NI for _ in tiles]
    for b in tiles:
        for s in lines:
            pivot = diag[b][s]
            if s > 0:
                pivot = pivot + w_w[b][s] * factors[b][s - 1]
            pivots[b][s] = 1.0 / pivot
            factors[b][s] = -w_e[b][s] * pivots[b][s]

    def precondition(r):
        out = []
        for b in tiles:
            part = []
            for s in lines:
                value = r[b][s]
                if s > 0:
                    value = value + w_w[b][s] * part[s - 1]
                part.append(value * pivots[b][s])
            for s in range(NI - 2, -1, -1):
                part[s] = part[s] - factors[b][s] * part[s + 1]
            out.append(part)
        return out

    x = load(1)
    drive = load(2)
    start = every(lambda h, d, a: jnp.where(h > 0.0, d, 0.0) - a, height, drive, apply(x))
    load = load_late()
    t_u = load(0)
    t_v = load(1)
    residual = every(
        lambda h, d, e, w, n, s: d - jnp.where(h > 0.0, 0.5 * DIVERGENCE * ((e - w) + (n - s)), 0.0),
        height, start, east(t_u), west(t_u), north(t_v, -1), south(t_v))
    mid = 0.5 * (SPECTRUM_HIGH + SPECTRUM_LOW)
    half = 0.5 * (SPECTRUM_HIGH - SPECTRUM_LOW)
    ratio = mid / half
    direction = every(lambda a: a / mid, precondition(residual))
    rho = 1.0 / ratio
    for step in range(ITERS):
        x = every(lambda a, b: a + b, x, direction)
        residual = every(lambda a, b: a - b, residual, apply(direction))
        if step + 1 < ITERS:
            rho_next = 1.0 / (2.0 * ratio - rho)
            keep, gain = rho_next * rho, 2.0 * rho_next / half
            direction = every(lambda d, z: keep * d + gain * z, direction, precondition(residual))
            rho = rho_next
    squares = every(lambda a: a * a, residual)
    total = functools.reduce(lambda a, b: a + b, [squares[b][s] for b in tiles for s in lines])
    total = jnp.sum(jnp.sum(total, axis=1, keepdims=True), axis=0, keepdims=True)
    rms = jnp.sqrt(total / cells + EPSILON)
    slope_x = every(lambda e, w: 0.5 * (e - w), east(x), west(x))
    slope_y = every(lambda n, s: 0.5 * (n - s), north(x, 1), south(x))
    return x, slope_x, slope_y, rms


def finish_kernel(t_ref, s_ref, u_ref, v_ref, x_ref, rms_ref, num_ref, sea_ref, ot_ref, os_ref, ou_ref,
                  ov_ref, ox_ref, orms_ref):
    depth = (num_ref[...] * sea_ref[...]).astype(F32)
    su = x_ref[1]
    sv = x_ref[2]
    for k in range(t_ref.shape[0]):
        wet = depth > k + 0.5
        ot_ref[k] = t_ref[k]
        os_ref[k] = s_ref[k]
        ou_ref[k] = jnp.where(wet, u_ref[k] - su, 0.0)
        ov_ref[k] = jnp.where(wet, v_ref[k] - sv, 0.0)
    ox_ref[...] = x_ref[0]
    orms_ref[0] = rms_ref[0]


def per_device(n_lon, n_lat, temp, salt, u, v, num, sea, thick, eta, drive):
    K, NI, NJ = temp.shape
    KC = 8 if K % 8 == 0 else K
    NC = K // KC
    n_half = n_lon * n_lat // 2
    vmem = pl.BlockSpec(memory_space=pltpu.VMEM)
    smem = pl.BlockSpec(memory_space=pltpu.SMEM)
    anywhere = pl.BlockSpec(memory_space=pltpu.HBM)
    big = jax.ShapeDtypeStruct((K, NI, NJ), F32)
    flat = jax.ShapeDtypeStruct((NI, NJ), F32)
    one = jax.ShapeDtypeStruct((1,), F32)
    args = (temp, salt, u, v, num, sea, thick, eta, drive)
    sides = pltpu.VMEM((NC, 6 * KC, NJ), F32)
    tile = pltpu.VMEM((NI, NJ), F32)
    parts = pl.pallas_call(
        functools.partial(step_kernel, n_lon, n_lat, KC),
        out_shape=(big, big, big, big, jax.ShapeDtypeStruct((3, NI, NJ), F32), one),
        in_specs=[anywhere] * 9,
        out_specs=(vmem,) * 5 + (smem,),
        scratch_shapes=[(pltpu.SMEM if a.ndim == 1 else pltpu.VMEM)(a.shape, a.dtype) for a in args] + [
            sides, sides, tile, tile,
            pltpu.VMEM((2, NI, NJ), F32), pltpu.VMEM((2, NI, NJ), F32),
            sides, sides, tile, tile,
            pltpu.VMEM((6, 2, NI, NJ), F32), pltpu.VMEM((8, max(KC, 2 * NI), NJ), F32),
            pltpu.VMEM((2, n_half, EARLY, NI, NJ), F32), pltpu.VMEM((2, n_half, LATE, NI, NJ), F32),
            pltpu.VMEM((3, n_lat, n_lon * NI, NJ), F32),
            pltpu.SemaphoreType.DMA((9,)),
            pltpu.SemaphoreType.DMA((8,)), pltpu.SemaphoreType.DMA((8,)),
            pltpu.SemaphoreType.DMA((2, NC)), pltpu.SemaphoreType.DMA((2, NC)),
            pltpu.SemaphoreType.DMA((4,)), pltpu.SemaphoreType.DMA((4,)),
        ],
        compiler_params=pltpu.CompilerParams(
            collective_id=0, has_side_effects=True, vmem_limit_bytes=40 * 1024 * 1024),
        name="step",
    )(*args)
    outs = pl.pallas_call(
        finish_kernel,
        out_shape=(big, big, big, big, flat, one),
        in_specs=[vmem] * 5 + [smem] + [vmem] * 2,
        out_specs=(vmem,) * 5 + (smem,),
        compiler_params=pltpu.CompilerParams(vmem_limit_bytes=16 * 1024 * 1024),
        name="finish",
    )(*parts, num, sea)
    return outs[:5] + (outs[5].reshape(()),)


def solution(mesh):
    n_lon, n_lat = mesh.shape["lon"], mesh.shape["lat"]
    spec3 = P(None, "lon", "lat")
    spec2 = P("lon", "lat")
    return jax.shard_map(
        functools.partial(per_device, n_lon, n_lat),
        mesh=mesh,
        in_specs=(spec3, spec3, spec3, spec3, spec2, spec2, P(), spec2, spec2),
        out_specs=(spec3, spec3, spec3, spec3, spec2, P()),
        check_vma=False,
    )
```

```python
import functools

import jax
import jax.numpy as jnp
from jax import lax
from jax.experimental import pallas as pl
from jax.experimental.pallas import tpu as pltpu
from jax.sharding import PartitionSpec as P

ITERS = 4
DIFFUSION = 0.15
MIXING = 0.1
EXPANSION = 0.2
CONTRACTION = 0.15
PRESSURE_SCALE = 0.02
CORIOLIS = 0.5
FRICTION = 0.01
DIVERGENCE = 0.3
STORAGE = 0.1
SPECTRUM_LOW = 0.1
SPECTRUM_HIGH = 1.9
GRAVITY = 0.3
EPSILON = 1e-06

MESH = pl.DeviceIdType.MESH
F32 = jnp.float32
SLOT_N, SLOT_NE, SLOT_NW, SLOT_S, SLOT_SE, SLOT_SW = range(6)
SEM_E, SEM_W = 6, 7
EARLY = 3
LATE = 2


def iota(shape, axis):
    return lax.broadcasted_iota(jnp.int32, shape, axis)


def flip_rows(x):
    n = x.shape[0]
    row = iota(x.shape, 0)
    bit = n // 2
    while bit:
        up = pltpu.roll(x, bit, 0)
        down = pltpu.roll(x, n - bit, 0)
        x = up if 2 * bit == n else jnp.where((row & bit) != 0, up, down)
        bit //= 2
    return x


def step_kernel(n_lon, n_lat, KC, *refs):
    sources, refs = refs[:9], refs[9:]
    targets, (ox_ref, orms_ref) = refs[:4], refs[4:6]
    inputs, refs = refs[6:15], refs[15:]
    t_ref, s_ref, u_ref, v_ref, num_ref, sea_ref, thick_ref, eta_ref, drive_ref = inputs
    (epk, wpk, ebase, wbase, npk, spk, slot_e, slot_w, base_e, base_w, slots, rim, early, late, held,
     ot_ref, os_ref, ou_ref, ov_ref, load_sem, store_sem, send_sem, recv_sem, side_send, side_recv, cast_send, cast_recv) = refs
    K, NI, NJ = t_ref.shape
    NC = K // KC
    loads = [pltpu.make_async_copy(src, dst, load_sem.at[i]) for i, (src, dst) in enumerate(zip(sources, inputs))]
    for load in loads[4:] + loads[:4]:
        load.start()
    p = lax.axis_index("lon")
    q = lax.axis_index("lat")
    east_dev = lax.rem(p + 1, n_lon)
    west_dev = lax.rem(p + n_lon - 1, n_lon)
    at_pole = q == n_lat - 1
    not_pole = q < n_lat - 1
    not_south = q > 0
    mirror = n_lon - 1 - p
    mirror_ne = lax.rem(2 * n_lon - 2 - p, n_lon)
    mirror_nw = lax.rem(2 * n_lon - p, n_lon)
    ne_remote = jnp.logical_or(not_pole, mirror_ne != p)
    nw_remote = jnp.logical_or(not_pole, mirror_nw != p)
    ne_self = jnp.logical_and(at_pole, mirror_ne == p)
    nw_self = jnp.logical_and(at_pole, mirror_nw == p)

    barrier = pltpu.get_barrier_semaphore()

    def greet(lon, lat):
        pl.semaphore_signal(barrier, inc=1, device_id={"lon": lon, "lat": lat}, device_id_type=MESH)

    greet(east_dev, q)
    greet(west_dev, q)

    @pl.when(not_south)
    def _():
        for lon in (p, east_dev, west_dev):
            greet(lon, q - 1)

    @pl.when(not_pole)
    def _():
        for lon in (p, east_dev, west_dev):
            greet(lon, q + 1)

    @pl.when(at_pole)
    def _():
        greet(mirror, q)

    @pl.when(jnp.logical_and(at_pole, mirror_ne != p))
    def _():
        greet(mirror_ne, q)

    @pl.when(jnp.logical_and(at_pole, mirror_nw != p))
    def _():
        greet(mirror_nw, q)

    parity = lax.rem(q, 2)
    partner = q + 1 - 2 * parity
    n_half = n_lon * n_lat // 2
    me_half = (q // 2) * n_lon + p

    def half_peer(r):
        other = lax.rem(me_half + r, n_half)
        return lax.rem(other, n_lon), 2 * (other // n_lon) + parity

    def greet_half(r, carry):
        greet(*half_peer(r))
        return carry

    lax.fori_loop(1, n_half, greet_half, 0)
    greet(p, partner)

    for load in loads:
        load.wait()
    sub = iota((NI, NJ), 0)
    lane = iota((NI, NJ), 1)
    depth = (num_ref[...] * sea_ref[...]).astype(F32)
    height = jnp.zeros((NI, NJ), F32)
    for k in range(K):
        height = height + jnp.where(depth > k + 0.5, thick_ref[k], 0.0)
    early[parity, me_half, 0] = height
    early[parity, me_half, 1] = sea_ref[...].astype(F32) * eta_ref[...]
    early[parity, me_half, 2] = drive_ref[...]

    fields = (t_ref, s_ref, u_ref, v_ref)
    for pk, base, d1, d2 in ((epk, ebase, NI - 1, NI - 2), (wpk, wbase, 0, 1)):
        for c in range(NC):
            levels = slice(c * KC, (c + 1) * KC)
            for f, (ref, d) in enumerate(((t_ref, d1), (s_ref, d1), (u_ref, d1), (v_ref, d1), (u_ref, d2), (v_ref, d2))):
                pk[c, f * KC:(f + 1) * KC, :] = ref[levels, d, :]
        base[...] = jnp.where(sub == 0, depth[d1:d1 + 1, :], depth[d2:d2 + 1, :])

    n0 = jnp.zeros((NI, NJ), F32)
    s0 = jnp.zeros((NI, NJ), F32)
    n1 = jnp.zeros((NI, NJ), F32)
    s1 = jnp.zeros((NI, NJ), F32)

    def put(acc, x, source, target):
        moved = pltpu.roll(x, (target - source) % NJ, 1) if source != target else x
        return jnp.where(lane == target, moved, acc)

    for f, ref in enumerate(fields):
        for k in range(K):
            x = ref[k]
            target = f * K + k
            n0 = put(n0, x, NJ - 1, target)
            s0 = put(s0, x, 0, target)
            if f >= 2:
                n1 = put(n1, x, NJ - 2, target)
                s1 = put(s1, x, 1, target)
    n1 = put(put(n1, depth, NJ - 1, 0), depth, NJ - 2, 1)
    s1 = put(put(s1, depth, 0, 0), depth, 1, 1)
    npk[0] = n0
    npk[1] = n1
    spk[0] = s0
    spk[1] = s1

    peers = (3 + n_half + 2 * not_pole.astype(jnp.int32) + 3 * not_south.astype(jnp.int32)
             + at_pole.astype(jnp.int32) * ((mirror_ne != p).astype(jnp.int32) + (mirror_nw != p).astype(jnp.int32)))
    pl.semaphore_wait(barrier, peers)

    def copy(src, dst, lon, lat, out, into):
        return pltpu.make_async_remote_copy(
            src_ref=src, dst_ref=dst, send_sem=out, recv_sem=into,
            device_id={"lon": lon, "lat": lat}, device_id_type=MESH)

    def edge(src, slot, lon, lat, out):
        return copy(src, slots.at[slot], lon, lat, send_sem.at[out], recv_sem.at[slot])

    def side_east(c):
        return copy(epk.at[c], slot_w.at[c], east_dev, q, side_send.at[0, c], side_recv.at[0, c])

    def side_west(c):
        return copy(wpk.at[c], slot_e.at[c], west_dev, q, side_send.at[1, c], side_recv.at[1, c])

    base_east = copy(ebase, base_w, east_dev, q, send_sem.at[SEM_E], recv_sem.at[SEM_W])
    base_west = copy(wbase, base_e, west_dev, q, send_sem.at[SEM_W], recv_sem.at[SEM_E])
    base_east.start()
    base_west.start()
    side_east(0).start()
    side_west(0).start()

    @pl.when(not_south)
    def _():
        edge(spk, SLOT_N, p, q - 1, SLOT_S).start()
        edge(spk, SLOT_NW, east_dev, q - 1, SLOT_SE).start()
        edge(spk, SLOT_NE, west_dev, q - 1, SLOT_SW).start()

    @pl.when(not_pole)
    def _():
        edge(npk, SLOT_S, p, q + 1, SLOT_N).start()
        edge(npk, SLOT_SW, east_dev, q + 1, SLOT_NE).start()
        edge(npk, SLOT_SE, west_dev, q + 1, SLOT_NW).start()

    @pl.when(at_pole)
    def _():
        edge(npk, SLOT_N, mirror, q, SLOT_N).start()

    @pl.when(jnp.logical_and(at_pole, mirror_ne != p))
    def _():
        edge(npk, SLOT_NE, mirror_ne, q, SLOT_NE).start()

    @pl.when(jnp.logical_and(at_pole, mirror_nw != p))
    def _():
        edge(npk, SLOT_NW, mirror_nw, q, SLOT_NW).start()

    def cast(buf, which):
        def send(r, carry):
            lon, lat = half_peer(r)
            mine = buf.at[parity, me_half]
            pltpu.make_async_remote_copy(
                src_ref=mine, dst_ref=mine, send_sem=cast_send.at[which], recv_sem=cast_recv.at[which],
                device_id={"lon": lon, "lat": lat}, device_id_type=MESH).start()
            return carry

        lax.fori_loop(1, n_half, send, 0)

    def cast_wait(buf, sem):
        rest = buf.at[parity, pl.ds(0, n_half - 1)]
        pltpu.make_async_copy(rest, rest, sem).wait()

    def hand_over(buf, which):
        return pltpu.make_async_remote_copy(
            src_ref=buf.at[parity], dst_ref=buf.at[parity], send_sem=cast_send.at[which],
            recv_sem=cast_recv.at[which], device_id={"lon": p, "lat": partner}, device_id_type=MESH)

    for c in range(1, NC):
        side_east(c).start()
        side_west(c).start()
    cast(early, 0)

    edge(npk, SLOT_N, p, q, SLOT_N).wait_recv()

    @pl.when(ne_remote)
    def _():
        edge(npk, SLOT_NE, p, q, SLOT_NE).wait_recv()

    @pl.when(nw_remote)
    def _():
        edge(npk, SLOT_NW, p, q, SLOT_NW).wait_recv()

    @pl.when(not_south)
    def _():
        for slot in (SLOT_S, SLOT_SE, SLOT_SW):
            edge(spk, slot, p, q, slot).wait_recv()

    sign = jnp.where(lane >= 2 * K, -1.0, 1.0).astype(F32)

    def northern(slot, own):
        out = []
        for i in range(2):
            x = slots[slot, i]
            if own is not None:
                x = jnp.where(own, npk[i], x)
            out.append(jnp.where(at_pole, flip_rows(x) * sign, x))
        return out

    def southern(slot):
        return [jnp.where(not_south, slots[slot, i], 0.0) for i in range(2)]

    pn0, pn1 = northern(SLOT_N, None)
    pne0, pne1 = northern(SLOT_NE, ne_self)
    pnw0, pnw1 = northern(SLOT_NW, nw_self)
    ps0, ps1 = southern(SLOT_S)
    pse0, pse1 = southern(SLOT_SE)
    psw0, psw1 = southern(SLOT_SW)

    def shift_e(x, row):
        return jnp.where(sub == NI - 1, row, pltpu.roll(x, NI - 1, 0))

    def shift_w(x, row):
        return jnp.where(sub == 0, row, pltpu.roll(x, 1, 0))

    level_l = (lane - K * (lane // K)).astype(F32) + 0.5

    def wet_l(d):
        return jnp.where(level_l < d, 1.0, 0.0)

    def spread(x, i):
        return jnp.broadcast_to(x[:, i:i + 1], (NI, NJ))

    def packed_lap(c0, c1, e0, e1, w0, w1, own, own_depth):
        d = spread(c1, 0)
        de = shift_e(d, jnp.broadcast_to(e1[0:1, 0:1], (NI, NJ)))
        dw = shift_w(d, jnp.broadcast_to(w1[NI - 1:NI, 0:1], (NI, NJ)))
        xe = shift_e(c0, jnp.broadcast_to(e0[0:1, :], (NI, NJ)))
        xw = shift_w(c0, jnp.broadcast_to(w0[NI - 1:NI, :], (NI, NJ)))
        total = wet_l(de) * (xe - c0) + wet_l(dw) * (xw - c0)
        total = total + wet_l(spread(c1, 1)) * (c1 - c0) + wet_l(own_depth) * (own - c0)
        return wet_l(d) * total

    lap_n = packed_lap(pn0, pn1, pne0, pne1, pnw0, pnw1, n0, spread(depth, NJ - 1))
    lap_s = packed_lap(ps0, ps1, pse0, pse1, psw0, psw1, s0, spread(depth, 0))
    rim[4, 0:NI, :] = lap_n
    rim[5, 0:NI, :] = lap_s
    rim[4, NI:2 * NI, :] = pn0
    rim[5, NI:2 * NI, :] = ps0

    base_east.wait_recv()
    base_west.wait_recv()

    row_c = iota((KC, NJ), 0)
    lane_c = iota((KC, NJ), 1)

    def wide(row):
        return jnp.broadcast_to(row, (KC, NJ))

    rim[6, 0:NI, :] = pne0
    rim[6, NI:2 * NI, :] = pse0
    rim[7, 0:NI, :] = pnw0
    rim[7, NI:2 * NI, :] = psw0
    side_depths = []
    for base, d1, cn1, cs1 in ((base_e, NI - 1, pne1[0:1], pse1[0:1]), (base_w, 0, pnw1[NI - 1:], psw1[NI - 1:])):
        d = wide(base[0:1, :])
        dn = jnp.where(lane_c == NJ - 1, jnp.broadcast_to(cn1[:, 0:1], (KC, NJ)), pltpu.roll(d, NJ - 1, 1))
        ds = jnp.where(lane_c == 0, jnp.broadcast_to(cs1[:, 0:1], (KC, NJ)), pltpu.roll(d, 1, 1))
        side_depths.append((d, wide(base[1:2, :]), wide(depth[d1:d1 + 1, :]), dn, ds))

    def side_laps(c):
        level_c = (row_c + c * KC).astype(F32) + 0.5
        for side, (slot, pk, corner) in enumerate(((slot_e, epk, 0), (slot_w, wpk, NI - 1))):
            mid, far, own, mn, ms = [jnp.where(level_c < d, 1.0, 0.0) for d in side_depths[side]]
            cn0 = rim[6 + side, corner:corner + 1, :]
            cs0 = rim[6 + side, NI + corner:NI + corner + 1, :]
            for i in range(2):
                f = 2 + i
                x = slot[c, f * KC:(f + 1) * KC, :]
                pick = lane_c == row_c + (c * KC + f * K)
                cn = jnp.sum(jnp.where(pick, wide(cn0), 0.0), axis=1, keepdims=True)
                cs = jnp.sum(jnp.where(pick, wide(cs0), 0.0), axis=1, keepdims=True)
                xn = jnp.where(lane_c == NJ - 1, jnp.broadcast_to(cn, (KC, NJ)), pltpu.roll(x, NJ - 1, 1))
                xs = jnp.where(lane_c == 0, jnp.broadcast_to(cs, (KC, NJ)), pltpu.roll(x, 1, 1))
                total = far * (slot[c, (4 + i) * KC:(5 + i) * KC, :] - x)
                total = total + own * (pk[c, f * KC:(f + 1) * KC, :] - x) + mn * (xn - x) + ms * (xs - x)
                rim[2 * side + i, 0:KC, :] = mid * total

    def shift_n(x, packed, source):
        return jnp.where(lane == NJ - 1, pltpu.roll(packed, NJ - 1 - source, 1), pltpu.roll(x, NJ - 1, 1))

    def shift_s(x, packed, source):
        return jnp.where(lane == 0, pltpu.roll(packed, lax.rem(NJ - source, NJ), 1), pltpu.roll(x, 1, 1))

    depth_e = shift_e(depth, base_e[0:1, :])
    depth_w = shift_w(depth, base_w[0:1, :])
    depth_n = shift_n(depth, pn1, 0)
    depth_s = jnp.where(lane == 0, ps1, pltpu.roll(depth, 1, 1))
    both_e = jnp.minimum(depth, depth_e)
    both_w = jnp.minimum(depth, depth_w)
    both_n = jnp.minimum(depth, depth_n)
    both_s = jnp.minimum(depth, depth_s)
    lat_index = (q * NJ + lane).astype(F32)
    coriolis = CORIOLIS * (2.0 * (lat_index + 0.5) / (n_lat * NJ) - 1.0)

    zero = jnp.zeros((NI, NJ), F32)

    def level(c, i, carry):
        k = c * KC + i
        inner = i
        pc, pe, pw, pn_, ps_, flux_t, flux_s, tu, tv = carry
        kf = lax.convert_element_type(k, F32) + 0.5
        h = thick_ref[k]
        nxt = jnp.minimum(k + 1, K - 1)
        h_next = thick_ref[nxt]
        hv = jnp.full((NI, NJ), h, F32)
        inv_space = 1.0 / (0.5 * (hv + h_next))
        inv_h = MIXING / hv

        def wet(d):
            return jnp.where(d > kf, 1.0, 0.0)

        mc = wet(depth)
        me, mw, mn, ms = wet(both_e), wet(both_w), wet(both_n), wet(both_s)
        below = jnp.where(jnp.logical_and(depth > kf + 1.0, k < K - 1), inv_space, 0.0)
        pn0v = rim[4, NI:2 * NI, :]
        ps0v = rim[5, NI:2 * NI, :]
        lapn = rim[4, 0:NI, :]
        laps = rim[5, 0:NI, :]

        def around(ref, f):
            x = ref[k]
            row = f * KC + inner
            return (x, shift_e(x, slot_e[c, row:row + 1, :]), shift_w(x, slot_w[c, row:row + 1, :]),
                    shift_n(x, pn0v, f * K + k), shift_s(x, ps0v, f * K + k))

        t = around(t_ref, 0)
        s = around(s_ref, 1)
        u = around(u_ref, 2)
        v = around(v_ref, 3)
        ae = 0.25 * me * (u[0] + u[1])
        aw = 0.25 * mw * (u[0] + u[2])
        an = 0.25 * mn * (v[0] + v[3])
        as_ = 0.25 * ms * (v[0] + v[4])
        ge, gw, gn, gs = DIFFUSION * me, DIFFUSION * mw, DIFFUSION * mn, DIFFUSION * ms

        def tracer(x, ref, flux_above):
            c, e, w, n, so = x
            total = aw * (w + c) - gw * (c - w) - ae * (c + e) + ge * (e - c)
            total = total + as_ * (so + c) - gs * (c - so) - an * (c + n) + gn * (n - c)
            flux = below * (ref[nxt] - c)
            return mc * (c + total + inv_h * (flux - flux_above)), flux

        new_t, flux_t = tracer(t, t_ref, flux_t)
        new_s, flux_s = tracer(s, s_ref, flux_s)
        ot_ref[k] = new_t
        os_ref[k] = new_s
        pressures = []
        for i, (acc, d) in enumerate(((pc, depth), (pe, depth_e), (pw, depth_w), (pn_, depth_n), (ps_, depth_s))):
            density = CONTRACTION * s[i] - EXPANSION * t[i]
            pressures.append(acc + jnp.where(d > kf, density * h, 0.0))
        pc, pe, pw, pn_, ps_ = pressures
        grad_x = 0.5 * (me * (pe - pc) + mw * (pc - pw))
        grad_y = 0.5 * (mn * (pn_ - pc) + ms * (pc - ps_))

        def biharmonic(x, i):
            c, e, w, n, so = x
            lap = me * (e - c) + mw * (w - c) + mn * (n - c) + ms * (so - c)
            le = shift_e(lap, rim[i, inner:inner + 1, :])
            lw = shift_w(lap, rim[2 + i, inner:inner + 1, :])
            source = (2 + i) * K + k
            ln = shift_n(lap, lapn, source)
            ls = shift_s(lap, laps, source)
            return me * (le - lap) + mw * (lw - lap) + mn * (ln - lap) + ms * (ls - lap)

        u_star = mc * (u[0] + coriolis * v[0] - PRESSURE_SCALE * grad_x - FRICTION * biharmonic(u, 0))
        v_star = mc * (v[0] - coriolis * u[0] - PRESSURE_SCALE * grad_y - FRICTION * biharmonic(v, 1))
        ou_ref[k] = u_star
        ov_ref[k] = v_star
        return (pc, pe, pw, pn_, ps_, flux_t, flux_s, tu + h * u_star, tv + h * v_star)

    def chunk(c, carry):
        side_east(c).wait_recv()
        side_west(c).wait_recv()
        side_laps(c)
        for i in range(KC):
            carry = level(c, i, carry)
        return carry

    carry = lax.fori_loop(0, NC, chunk, (zero,) * 9)
    late[parity, me_half, 0] = carry[7]
    late[parity, me_half, 1] = carry[8]
    cast(late, 1)
    stores = [pltpu.make_async_copy(src, dst, store_sem.at[i])
              for i, (src, dst) in enumerate(zip((ot_ref, os_ref, ou_ref, ov_ref), targets))]
    for store in stores:
        store.start()

    cast_wait(early, cast_recv.at[0])
    early_over = hand_over(early, 2)
    early_over.start()
    early_over.wait_recv()

    def loader(buf, count):
        flat = buf.reshape(2 * n_half * count * NI, NJ)

        def load(f):
            return [[flat[pl.ds((((b % 2) * n_half + (b // 2) * n_lon) * count + f) * NI + s, n_lon,
                                stride=count * NI), :] for s in range(NI)] for b in range(n_lat)]

        return load

    def late_loader():
        cast_wait(late, cast_recv.at[1])
        late_over = hand_over(late, 3)
        late_over.start()
        late_over.wait_recv()
        return loader(late, LATE)

    x, slope_x, slope_y, rms = surface_solve(loader(early, EARLY), late_loader, n_lon, n_lat, K, NI, NJ,
                                             n_lon * NI * n_lat * NJ)
    for i, field in enumerate((x, slope_x, slope_y)):
        for b in range(n_lat):
            for s in range(NI):
                held[i, b, pl.ds(s, n_lon, stride=NI), :] = field[b][s]
    orms_ref[0] = jnp.max(jnp.broadcast_to(rms, (8, 128)))
    block = pl.ds(pl.multiple_of(p * NI, NI), NI)
    ox_ref[0] = held[0, q, block, :]
    ox_ref[1] = GRAVITY * held[1, q, block, :]
    ox_ref[2] = GRAVITY * held[2, q, block, :]

    for store in stores:
        store.wait()
    cast_wait(early, cast_send.at[0])
    cast_wait(late, cast_send.at[1])
    early_over.wait_send()
    hand_over(late, 3).wait_send()

    base_east.wait_send()
    base_west.wait_send()
    for c in range(NC):
        side_east(c).wait_send()
        side_west(c).wait_send()

    @pl.when(not_south)
    def _():
        for out in (SLOT_S, SLOT_SE, SLOT_SW):
            edge(spk, SLOT_N, p, q, out).wait_send()

    edge(npk, SLOT_N, p, q, SLOT_N).wait_send()

    @pl.when(ne_remote)
    def _():
        edge(npk, SLOT_NE, p, q, SLOT_NE).wait_send()

    @pl.when(nw_remote)
    def _():
        edge(npk, SLOT_NW, p, q, SLOT_NW).wait_send()


def surface_solve(load, load_late, n_lon, n_lat, K, NI, NJ, cells):
    tiles = range(n_lat)
    lines = range(NI)
    lane = iota((n_lon, NJ), 1)

    def every(fn, *arrays):
        return [[fn(*(a[b][s] for a in arrays)) for s in lines] for b in tiles]

    def east(x):
        return [x[b][1:] + [pltpu.roll(x[b][0], n_lon - 1, 0)] for b in tiles]

    def west(x):
        return [[pltpu.roll(x[b][NI - 1], 1, 0)] + x[b][:-1] for b in tiles]

    def north(x, sign):
        out = []
        for b in tiles:
            row = []
            for s in lines:
                if b + 1 < n_lat:
                    beyond = pltpu.roll(x[b + 1][s], NJ - 1, 1)
                else:
                    beyond = flip_rows(x[b][NI - 1 - s])
                    beyond = -beyond if sign < 0 else beyond
                row.append(jnp.where(lane == NJ - 1, beyond, pltpu.roll(x[b][s], NJ - 1, 1)))
            out.append(row)
        return out

    def south(x):
        out = []
        for b in tiles:
            row = []
            for s in lines:
                beyond = pltpu.roll(x[b - 1][s], 1, 1) if b > 0 else 0.0
                row.append(jnp.where(lane == 0, beyond, pltpu.roll(x[b][s], 1, 1)))
            out.append(row)
        return out

    height = load(0)
    scale = lambda a, c: jnp.minimum(a, c) * (1.0 / K)
    w_e = every(scale, height, east(height))
    w_w = every(scale, height, west(height))
    w_n = every(scale, height, north(height, 1))
    w_s = every(scale, height, south(height))
    diag = every(lambda a, b, c, d: STORAGE + a + b + c + d, w_e, w_w, w_n, w_s)

    def apply(x):
        return every(
            lambda dg, c, we, e, ww, w, wn, n, ws, s: dg * c - (we * e + ww * w + wn * n + ws * s),
            diag, x, w_e, east(x), w_w, west(x), w_n, north(x, 1), w_s, south(x))

    factors = [[None] * NI for _ in tiles]
    pivots = [[None] * NI for _ in tiles]
    for b in tiles:
        for s in lines:
            pivot = diag[b][s]
            if s > 0:
                pivot = pivot + w_w[b][s] * factors[b][s - 1]
            pivots[b][s] = 1.0 / pivot
            factors[b][s] = -w_e[b][s] * pivots[b][s]

    def precondition(r):
        out = []
        for b in tiles:
            part = []
            for s in lines:
                value = r[b][s]
                if s > 0:
                    value = value + w_w[b][s] * part[s - 1]
                part.append(value * pivots[b][s])
            for s in range(NI - 2, -1, -1):
                part[s] = part[s] - factors[b][s] * part[s + 1]
            out.append(part)
        return out

    x = load(1)
    drive = load(2)
    start = every(lambda h, d, a: jnp.where(h > 0.0, d, 0.0) - a, height, drive, apply(x))
    load = load_late()
    t_u = load(0)
    t_v = load(1)
    residual = every(
        lambda h, d, e, w, n, s: d - jnp.where(h > 0.0, 0.5 * DIVERGENCE * ((e - w) + (n - s)), 0.0),
        height, start, east(t_u), west(t_u), north(t_v, -1), south(t_v))
    mid = 0.5 * (SPECTRUM_HIGH + SPECTRUM_LOW)
    half = 0.5 * (SPECTRUM_HIGH - SPECTRUM_LOW)
    ratio = mid / half
    direction = every(lambda a: a / mid, precondition(residual))
    rho = 1.0 / ratio
    for step in range(ITERS):
        x = every(lambda a, b: a + b, x, direction)
        residual = every(lambda a, b: a - b, residual, apply(direction))
        if step + 1 < ITERS:
            rho_next = 1.0 / (2.0 * ratio - rho)
            keep, gain = rho_next * rho, 2.0 * rho_next / half
            direction = every(lambda d, z: keep * d + gain * z, direction, precondition(residual))
            rho = rho_next
    squares = every(lambda a: a * a, residual)
    total = functools.reduce(lambda a, b: a + b, [squares[b][s] for b in tiles for s in lines])
    total = jnp.sum(jnp.sum(total, axis=1, keepdims=True), axis=0, keepdims=True)
    rms = jnp.sqrt(total / cells + EPSILON)
    slope_x = every(lambda e, w: 0.5 * (e - w), east(x), west(x))
    slope_y = every(lambda n, s: 0.5 * (n - s), north(x, 1), south(x))
    return x, slope_x, slope_y, rms


def finish_kernel(t_ref, s_ref, u_ref, v_ref, x_ref, rms_ref, num_ref, sea_ref, ot_ref, os_ref, ou_ref,
                  ov_ref, ox_ref, orms_ref):
    depth = (num_ref[...] * sea_ref[...]).astype(F32)
    su = x_ref[1]
    sv = x_ref[2]
    for k in range(t_ref.shape[0]):
        wet = depth > k + 0.5
        ot_ref[k] = t_ref[k]
        os_ref[k] = s_ref[k]
        ou_ref[k] = jnp.where(wet, u_ref[k] - su, 0.0)
        ov_ref[k] = jnp.where(wet, v_ref[k] - sv, 0.0)
    ox_ref[...] = x_ref[0]
    orms_ref[0] = rms_ref[0]


def per_device(n_lon, n_lat, temp, salt, u, v, num, sea, thick, eta, drive):
    K, NI, NJ = temp.shape
    KC = 8 if K % 8 == 0 else K
    NC = K // KC
    n_half = n_lon * n_lat // 2
    vmem = pl.BlockSpec(memory_space=pltpu.VMEM)
    smem = pl.BlockSpec(memory_space=pltpu.SMEM)
    anywhere = pl.BlockSpec(memory_space=pltpu.HBM)
    big = jax.ShapeDtypeStruct((K, NI, NJ), F32)
    flat = jax.ShapeDtypeStruct((NI, NJ), F32)
    one = jax.ShapeDtypeStruct((1,), F32)
    args = (temp, salt, u, v, num, sea, thick, eta, drive)
    sides = pltpu.VMEM((NC, 6 * KC, NJ), F32)
    tile = pltpu.VMEM((NI, NJ), F32)
    parts = pl.pallas_call(
        functools.partial(step_kernel, n_lon, n_lat, KC),
        out_shape=(big, big, big, big, jax.ShapeDtypeStruct((3, NI, NJ), F32), one),
        in_specs=[anywhere] * 9,
        out_specs=(anywhere,) * 4 + (vmem, smem),
        scratch_shapes=[(pltpu.SMEM if a.ndim == 1 else pltpu.VMEM)(a.shape, a.dtype) for a in args] + [
            sides, sides, tile, tile,
            pltpu.VMEM((2, NI, NJ), F32), pltpu.VMEM((2, NI, NJ), F32),
            sides, sides, tile, tile,
            pltpu.VMEM((6, 2, NI, NJ), F32), pltpu.VMEM((8, max(KC, 2 * NI), NJ), F32),
            pltpu.VMEM((2, n_half, EARLY, NI, NJ), F32), pltpu.VMEM((2, n_half, LATE, NI, NJ), F32),
            pltpu.VMEM((3, n_lat, n_lon * NI, NJ), F32),
            pltpu.VMEM((K, NI, NJ), F32), pltpu.VMEM((K, NI, NJ), F32),
            pltpu.VMEM((K, NI, NJ), F32), pltpu.VMEM((K, NI, NJ), F32),
            pltpu.SemaphoreType.DMA((9,)), pltpu.SemaphoreType.DMA((4,)),
            pltpu.SemaphoreType.DMA((8,)), pltpu.SemaphoreType.DMA((8,)),
            pltpu.SemaphoreType.DMA((2, NC)), pltpu.SemaphoreType.DMA((2, NC)),
            pltpu.SemaphoreType.DMA((4,)), pltpu.SemaphoreType.DMA((4,)),
        ],
        compiler_params=pltpu.CompilerParams(
            collective_id=0, has_side_effects=True),
        name="step",
    )(*args)
    outs = pl.pallas_call(
        finish_kernel,
        out_shape=(big, big, big, big, flat, one),
        in_specs=[vmem] * 5 + [smem] + [vmem] * 2,
        out_specs=(vmem,) * 5 + (smem,),
        name="finish",
    )(*parts, num, sea)
    return outs[:5] + (outs[5].reshape(()),)


def solution(mesh):
    n_lon, n_lat = mesh.shape["lon"], mesh.shape["lat"]
    spec3 = P(None, "lon", "lat")
    spec2 = P("lon", "lat")
    return jax.shard_map(
        functools.partial(per_device, n_lon, n_lat),
        mesh=mesh,
        in_specs=(spec3, spec3, spec3, spec3, spec2, spec2, P(), spec2, spec2),
        out_specs=(spec3, spec3, spec3, spec3, spec2, P()),
        check_vma=False,
    )
```
